8 devices in a mesh: dp: 2 (over z, y), tp: 4 (over x, core).
Axes of the slice: x: 2, y: 2, z: 1, core: 2. Of those that a mesh axis runs over, the one named last changes fastest.
Arguments:
- tokens: int32 [2, 768], P('dp'), parts along dimension 0
- positions: int32 [2, 768], P('dp'), parts along dimension 0
- embed_table: bfloat16 [262208, 2560], P('tp')
- w_query: bfloat16 [2560, 8, 256], P(None, 'tp')
- w_key: bfloat16 [2560, 4, 256], P(None, 'tp')
- w_value: bfloat16 [2560, 4, 256], P(None, 'tp')
- w_out: bfloat16 [8, 256, 2560], P('tp')
- w_gate: bfloat16 [2560, 10240], P(None, 'tp')
- w_up: bfloat16 [2560, 10240], P(None, 'tp')
- w_down: bfloat16 [10240, 2560], P('tp')
- norm_pre_att: float32 [2560], replicated
- norm_post_att: float32 [2560], replicated
- norm_pre_ffw: float32 [2560], replicated
- norm_post_ffw: float32 [2560], replicated
Outputs:
- output: bfloat16 [2, 768, 2560], P('dp', 'tp'), parts along dimension 0
There are 2 independent parts. The reference program is written for one: setup_inputs(seed, part) draws one part's arguments, and reference() takes and returns one part's arrays. A program takes and returns all parts, laid end to end along the dimension named above; an argument that names none is the same for every part.
All inputs are finite; a program needn't handle non-finite values.
Results may differ from the reference program's by a relative error of at most 0.02.
Values are sent between devices in bfloat16 or wider.
A program may use at most 1.5 GiB of HBM per device.

```python
import jax
import jax.numpy as jnp
from jax import lax

BATCH_SIZE = 1
SEQ_LEN = 768
MODEL_DIM = 2560
N_HEADS = 8
KV_HEADS = 4
HEAD_DIM = 256
FFN_DIM = 10240
VOCAB_SIZE = 262208
WINDOW = 4096
QUERY_SCALAR = 256

GROUP_SIZE = N_HEADS // KV_HEADS
QUERY_BLOCK = min(128, SEQ_LEN)
KEY_SPAN = min(SEQ_LEN, WINDOW + QUERY_BLOCK)
SOFT_CAP = 50.0
NORM_EPS = 1e-6
ROPE_BASE = 10000.0


def setup_inputs(seed: int = 0, part: int = 0) -> dict:
    root_key = jax.random.key(seed)
    key_list = jax.random.split(root_key, 11)
    part_keys = jax.random.split(jax.random.fold_in(root_key, part), 5)
    grid_shape = (BATCH_SIZE, SEQ_LEN)
    choice = jax.random.randint(part_keys[0], grid_shape, 0, 4, dtype=jnp.int32)
    hot_ids = jax.random.randint(part_keys[1], grid_shape, 0, VOCAB_SIZE // 4, dtype=jnp.int32)
    any_ids = jax.random.randint(part_keys[2], grid_shape, 0, VOCAB_SIZE, dtype=jnp.int32)
    tokens = jnp.where(choice < 3, hot_ids, any_ids)
    tokens = tokens.at[0, 0].set(VOCAB_SIZE - 1).at[0, 1].set(0)
    pos_step = max(1, (2 * WINDOW) // SEQ_LEN)
    pos_gaps = jax.random.randint(part_keys[3], grid_shape, 1, 2 * pos_step + 1, dtype=jnp.int32)
    first_pos = jax.random.randint(part_keys[4], (BATCH_SIZE, 1), 0, WINDOW, dtype=jnp.int32)
    positions = (first_pos + jnp.cumsum(pos_gaps, axis=1) - pos_gaps[:, :1]).astype(jnp.int32)

    def draw_weight(key_index, w_shape, fan_in):
        raw_noise = jax.random.normal(key_list[key_index], w_shape, jnp.float32)
        return (raw_noise * fan_in ** -0.5).astype(jnp.bfloat16)

    def table_rows(row_group):
        raw_noise = jax.random.normal(jax.random.fold_in(key_list[0], row_group), (VOCAB_SIZE // 8, MODEL_DIM), jnp.float32)
        return (raw_noise * MODEL_DIM ** -0.5).astype(jnp.bfloat16)

    embed_table = lax.map(table_rows, jnp.arange(8)).reshape(VOCAB_SIZE, MODEL_DIM)
    norm_draws = 0.3 * jax.random.normal(key_list[8], (4, MODEL_DIM), jnp.float32)
    return {
        "tokens": tokens,
        "positions": positions,
        "embed_table": embed_table,
        "w_query": draw_weight(1, (MODEL_DIM, N_HEADS, HEAD_DIM), MODEL_DIM),
        "w_key": draw_weight(2, (MODEL_DIM, KV_HEADS, HEAD_DIM), MODEL_DIM),
        "w_value": draw_weight(3, (MODEL_DIM, KV_HEADS, HEAD_DIM), MODEL_DIM),
        "w_out": draw_weight(4, (N_HEADS, HEAD_DIM, MODEL_DIM), N_HEADS * HEAD_DIM),
        "w_gate": draw_weight(5, (MODEL_DIM, FFN_DIM), MODEL_DIM),
        "w_up": draw_weight(6, (MODEL_DIM, FFN_DIM), MODEL_DIM),
        "w_down": draw_weight(7, (FFN_DIM, MODEL_DIM), FFN_DIM),
        "norm_pre_att": norm_draws[0],
        "norm_post_att": norm_draws[1],
        "norm_pre_ffw": norm_draws[2],
        "norm_post_ffw": norm_draws[3],
    }


def rms_norm(hidden, norm_scale):
    hidden = hidden.astype(jnp.float32)
    mean_sq = jnp.mean(hidden * hidden, axis=-1, keepdims=True)
    return (hidden * lax.rsqrt(mean_sq + NORM_EPS) * (1.0 + norm_scale)).astype(jnp.bfloat16)


def apply_rope(states, positions):
    half_dim = HEAD_DIM // 2
    inv_freq = ROPE_BASE ** (-2.0 * jnp.arange(half_dim, dtype=jnp.float32) / HEAD_DIM)
    angles = positions.astype(jnp.float32)[:, :, None] * inv_freq
    cos_tab = jnp.cos(angles)[:, :, None, :]
    sin_tab = jnp.sin(angles)[:, :, None, :]
    lower_half = states[..., :half_dim]
    upper_half = states[..., half_dim:]
    return jnp.concatenate([lower_half * cos_tab - upper_half * sin_tab, upper_half * cos_tab + lower_half * sin_tab], axis=-1)


def project(act_rows, weight, out_shape):
    flat_rows = act_rows.reshape(-1, act_rows.shape[-1])
    flat_w = weight.reshape(act_rows.shape[-1], -1)
    return jnp.dot(flat_rows, flat_w, preferred_element_type=jnp.float32).reshape(out_shape)


def attend(q_states, k_states, v_states, positions):
    n_blocks = SEQ_LEN // QUERY_BLOCK

    def one_block(block_idx):
        q_start = block_idx * QUERY_BLOCK
        k_start = jnp.maximum(q_start + QUERY_BLOCK - KEY_SPAN, 0)
        q_blk = lax.dynamic_slice_in_dim(q_states, q_start, QUERY_BLOCK, axis=1)
        k_blk = lax.dynamic_slice_in_dim(k_states, k_start, KEY_SPAN, axis=1)
        v_blk = lax.dynamic_slice_in_dim(v_states, k_start, KEY_SPAN, axis=1)
        q_pos = lax.dynamic_slice_in_dim(positions, q_start, QUERY_BLOCK, axis=1)
        k_pos = lax.dynamic_slice_in_dim(positions, k_start, KEY_SPAN, axis=1)
        scores = jnp.einsum("bqkgd,blkd->bkgql", q_blk.astype(jnp.float32), k_blk.astype(jnp.float32))
        capped = SOFT_CAP * jnp.tanh(scores / SOFT_CAP)
        offset = q_pos[:, :, None] - k_pos[:, None, :]
        keep_mask = (offset >= 0) & (offset < WINDOW)
        capped = jnp.where(keep_mask[:, None, None, :, :], capped, -1e30)
        att_probs = jax.nn.softmax(capped, axis=-1).astype(jnp.bfloat16)
        att_mix = jnp.einsum("bkgql,blkd->bqkgd", att_probs.astype(jnp.float32), v_blk.astype(jnp.float32))
        return att_mix.astype(jnp.bfloat16)

    blocks = lax.map(one_block, jnp.arange(n_blocks))
    return jnp.moveaxis(blocks, 0, 1).reshape(BATCH_SIZE, SEQ_LEN, KV_HEADS, GROUP_SIZE, HEAD_DIM)


def reference(tokens, positions, embed_table, w_query, w_key, w_value, w_out, w_gate, w_up, w_down, norm_pre_att, norm_post_att, norm_pre_ffw, norm_post_ffw):
    normalizer = jnp.sqrt(jnp.float32(MODEL_DIM)).astype(jnp.bfloat16).astype(jnp.float32)
    looked = jnp.take(embed_table, tokens, axis=0)
    embeds = (looked.astype(jnp.float32) * normalizer).astype(jnp.bfloat16)
    attn_in = rms_norm(embeds, norm_pre_att)
    heads_shape = (BATCH_SIZE, SEQ_LEN, N_HEADS, HEAD_DIM)
    kv_shape = (BATCH_SIZE, SEQ_LEN, KV_HEADS, HEAD_DIM)
    q_states = apply_rope(project(attn_in, w_query, heads_shape), positions) * QUERY_SCALAR ** -0.5
    q_states = q_states.astype(jnp.bfloat16).reshape(BATCH_SIZE, SEQ_LEN, KV_HEADS, GROUP_SIZE, HEAD_DIM)
    k_states = apply_rope(project(attn_in, w_key, kv_shape), positions).astype(jnp.bfloat16)
    v_states = project(attn_in, w_value, kv_shape).astype(jnp.bfloat16)
    att_mix = attend(q_states, k_states, v_states, positions)
    model_shape = (BATCH_SIZE, SEQ_LEN, MODEL_DIM)
    att_flat = att_mix.reshape(BATCH_SIZE, SEQ_LEN, N_HEADS * HEAD_DIM)
    att_proj = project(att_flat, w_out, model_shape).astype(jnp.bfloat16)
    resid_one = (embeds.astype(jnp.float32) + rms_norm(att_proj, norm_post_att).astype(jnp.float32)).astype(jnp.bfloat16)
    mlp_in = rms_norm(resid_one, norm_pre_ffw)
    ffn_shape = (BATCH_SIZE, SEQ_LEN, FFN_DIM)
    gate_pre = project(mlp_in, w_gate, ffn_shape)
    up_proj = project(mlp_in, w_up, ffn_shape)
    ffn_act = (jax.nn.gelu(gate_pre, approximate=True) * up_proj).astype(jnp.bfloat16)
    down_proj = project(ffn_act, w_down, model_shape).astype(jnp.bfloat16)
    return (resid_one.astype(jnp.float32) + rms_norm(down_proj, norm_post_ffw).astype(jnp.float32)).astype(jnp.bfloat16)
```

```python
import functools

import jax
import jax.numpy as jnp
from jax import lax
from jax.experimental import pallas as pl
from jax.experimental.pallas import tpu as pltpu
from jax.sharding import PartitionSpec as P

WINDOW = 4096
QUERY_SCALE = 256.0 ** -0.5
SOFT_CAP = 50.0
NORM_EPS = 1e-6
ROPE_BASE = 10000.0

N_CHUNK = 6
ROWS = 128
HALF = 64
SUB = 16
N_TILE = 512
MESH = pl.DeviceIdType.MESH
F32 = jnp.float32
BF16 = jnp.bfloat16


def rms(block, gain):
    mean_sq = jnp.mean(block * block, axis=-1, keepdims=True)
    return block * lax.rsqrt(mean_sq + NORM_EPS) * gain


def layer_kernel(
    part_ref, cos_ref, sin_ref, qpos_ref, kpos_ref,
    wq_hbm, wk_hbm, wv_hbm, wo_hbm, wg_hbm, wu_hbm, wd_hbm,
    g1_ref, g2_ref, g3_ref, g4_ref,
    out_ref,
    wq, wk, wv, wo, wg, wu, wd,
    own, sib, res, y_in, norm, k_all, v_all, o_buf, h_buf, pair_out, pair_in, z_in, stage,
    w_sem, own_sem, sib_ss, sib_rs, ex_ss, ex_rs, a_ss, a_rs, yp_ss, yp_rs,
    yx_ss, yx_rs, m_ss, m_rs, zp_ss, zp_rs, zx_ss, zx_rs, out_ss, out_rs,
):
    dp = lax.axis_index("dp")
    tp = lax.axis_index("tp")
    chip = lax.div(tp, 2)
    core = lax.rem(tp, 2)
    mate = 2 * chip + 1 - core
    far = 2 * (1 - chip) + core

    def remote(src, dst, send_sem, recv_sem, target):
        return pltpu.make_async_remote_copy(
            src_ref=src, dst_ref=dst, send_sem=send_sem, recv_sem=recv_sem,
            device_id=(dp, target), device_id_type=MESH)

    def half_rows(t):
        return pl.ds(pl.multiple_of(t * HALF, HALF), HALF)

    mine = pl.ds(pl.multiple_of(core * HALF, HALF), HALF)
    theirs = pl.ds(pl.multiple_of((1 - core) * HALF, HALF), HALF)

    def own_copy(t):
        rows = pl.ds(pl.multiple_of(t * ROWS + core * HALF, HALF), HALF)
        return pltpu.make_async_copy(part_ref.at[rows], own.at[half_rows(t)], own_sem.at[t])

    def sib_copy(t):
        rows = pl.ds(pl.multiple_of(t * ROWS + (1 - core) * HALF, HALF), HALF)
        return remote(part_ref.at[rows], sib.at[half_rows(t)], sib_ss.at[t], sib_rs.at[t], mate)

    def ex_copy(t):
        return remote(own.at[half_rows(t)], res.at[half_rows(t)], ex_ss.at[t], ex_rs.at[t], far)

    def norm_copy(slot, send_sem, recv_sem):
        return remote(norm.at[slot, mine], norm.at[slot, mine], send_sem, recv_sem, mate)

    def yp_copy():
        return remote(pair_out, pair_in.at[0], yp_ss, yp_rs, mate)

    def yx_copy(t):
        return remote(sib.at[half_rows(t)], y_in.at[half_rows(t)], yx_ss.at[t], yx_rs.at[t], far)

    def m_copy(t):
        slot = lax.rem(t, 2)
        return norm_copy(slot, m_ss.at[slot], m_rs.at[slot])

    def zp_copy(t):
        slot = lax.rem(t, 2)
        return remote(pair_out, pair_in.at[slot], zp_ss, zp_rs.at[slot], mate)

    def zx_copy(t):
        j = lax.rem(t, 3)
        return remote(own.at[half_rows(t)], z_in.at[half_rows(j)], zx_ss.at[j], zx_rs.at[j], far)

    weights = [
        pltpu.make_async_copy(src, dst, w_sem.at[i])
        for i, (src, dst) in enumerate(
            [(wq_hbm, wq), (wk_hbm, wk), (wv_hbm, wv), (wo_hbm, wo), (wg_hbm, wg), (wu_hbm, wu), (wd_hbm, wd)])
    ]

    barrier = pltpu.get_barrier_semaphore()
    for peer in (mate, far):
        pl.semaphore_signal(barrier, inc=1, device_id=(dp, peer), device_id_type=MESH)
    pl.semaphore_wait(barrier, 2)

    for t in range(N_CHUNK):
        sib_copy(t).start()
        own_copy(t).start()
    for copy in weights:
        copy.start()

    def sub_rows(base, i):
        return pl.ds(pl.multiple_of(base + i * SUB, SUB), SUB)

    def combine(dst, other, dst_base, other_base):
        def step(i, carry):
            rows = sub_rows(dst_base, i)
            total = dst[rows, :].astype(F32) + other[sub_rows(other_base, i), :].astype(F32)
            dst[rows, :] = total.astype(BF16)
            return carry
        lax.fori_loop(0, HALF // SUB, step, 0)

    def send_embed(t, carry):
        own_copy(t).wait()
        sib_copy(t).wait_recv()
        combine(own, sib, t * HALF, t * HALF)
        ex_copy(t).start()
        return carry
    lax.fori_loop(0, N_CHUNK, send_embed, 0)

    k_all[...] = jnp.zeros_like(k_all)
    v_all[...] = jnp.zeros_like(v_all)
    gain1 = 1.0 + g1_ref[...]
    gain2 = 1.0 + g2_ref[...]
    gain3 = 1.0 + g3_ref[...]
    gain4 = 1.0 + g4_ref[...]
    for t in range(N_CHUNK):
        sib_copy(t).wait_send()
    for copy in weights[:4]:
        copy.wait()

    def rope(states, cos_tab, sin_tab):
        lower, upper = states[:, :128], states[:, 128:]
        return lower * cos_tab - upper * sin_tab, upper * cos_tab + lower * sin_tab

    def attention_chunk(t, carry):
        base = t * HALF
        ex_copy(t).wait_recv()

        def embed_step(i, c):
            rows = sub_rows(base, i)
            embed = own[rows, :].astype(F32) + res[rows, :].astype(F32)
            res[rows, :] = embed.astype(BF16)
            norm[0, sub_rows(core * HALF, i), :] = rms(embed, gain1).astype(BF16)
            return c
        lax.fori_loop(0, HALF // SUB, embed_step, 0)

        copy = norm_copy(0, a_ss, a_rs)
        copy.start()
        copy.wait()
        act = norm[0]
        rows = pl.ds(pl.multiple_of(t * ROWS, ROWS), ROWS)
        cos_tab, sin_tab = cos_ref[rows, :], sin_ref[rows, :]
        lower, upper = rope(jnp.dot(act, wk[...], preferred_element_type=F32), cos_tab, sin_tab)
        k_all[rows, :128] = lower.astype(BF16)
        k_all[rows, 128:] = upper.astype(BF16)
        v_all[rows, :] = jnp.dot(act, wv[...], preferred_element_type=F32).astype(BF16)
        offset = qpos_ref[rows, :1] - kpos_ref[...]
        keep = (offset >= 0) & (offset < WINDOW)
        for head in range(2):
            proj = jnp.dot(act, wq[:, head * 256:(head + 1) * 256], preferred_element_type=F32)
            lower, upper = rope(proj, cos_tab, sin_tab)
            query = jnp.concatenate([(lower * QUERY_SCALE).astype(BF16), (upper * QUERY_SCALE).astype(BF16)], axis=-1)
            scores = lax.dot_general(query, k_all[...], (((1,), (1,)), ((), ())), preferred_element_type=F32)
            weight = jnp.where(keep, jnp.exp(SOFT_CAP * jnp.tanh(scores * (1.0 / SOFT_CAP))), 0.0)
            weight = weight * (1.0 / jnp.sum(weight, axis=-1, keepdims=True))
            mixed = jnp.dot(weight.astype(BF16), v_all[...], preferred_element_type=F32)
            o_buf[:, head * 256:(head + 1) * 256] = mixed.astype(BF16)

        def out_tile(n, c):
            cols = pl.ds(pl.multiple_of(n * N_TILE, N_TILE), N_TILE)
            sib[half_rows(t), cols] = jnp.dot(o_buf[mine, :], wo[:, cols], preferred_element_type=F32).astype(BF16)
            pair_out[:, cols] = jnp.dot(o_buf[theirs, :], wo[:, cols], preferred_element_type=F32).astype(BF16)
            return c
        lax.fori_loop(0, 2560 // N_TILE, out_tile, 0)
        copy = yp_copy()
        copy.start()
        copy.wait()
        combine(sib, pair_in.at[0], base, 0)
        yx_copy(t).start()
        return carry
    lax.fori_loop(0, N_CHUNK, attention_chunk, 0)

    for t in range(N_CHUNK):
        ex_copy(t).wait_send()
    for copy in weights[4:]:
        copy.wait()

    def mlp_in(t):
        base = t * HALF
        slot = lax.rem(t, 2)
        yx_copy(t).wait_recv()

        def step(i, c):
            rows = sub_rows(base, i)
            proj = (sib[rows, :].astype(F32) + y_in[rows, :].astype(F32)).astype(BF16).astype(F32)
            resid = (res[rows, :].astype(F32) + rms(proj, gain2).astype(BF16).astype(F32)).astype(BF16)
            res[rows, :] = resid
            norm[slot, sub_rows(core * HALF, i), :] = rms(resid.astype(F32), gain3).astype(BF16)
            return c
        lax.fori_loop(0, HALF // SUB, step, 0)
        m_copy(t).start()

    def finish_pair(t):
        zp_copy(t).wait_recv()
        combine(own, pair_in.at[lax.rem(t, 2)], t * HALF, 0)

        @pl.when(lax.div(t, 3) != chip)
        def _():
            zx_copy(t).start()

    mlp_in(0)

    def mlp_chunk(t, carry):
        slot = lax.rem(t, 2)
        m_copy(t).wait()

        def gate_tile(n, c):
            cols = pl.ds(pl.multiple_of(n * N_TILE, N_TILE), N_TILE)
            gate = jnp.dot(norm[slot], wg[:, cols], preferred_element_type=F32)
            up = jnp.dot(norm[slot], wu[:, cols], preferred_element_type=F32)
            h_buf[:, cols] = (jax.nn.gelu(gate, approximate=True) * up).astype(BF16)
            return c
        lax.fori_loop(0, 2560 // N_TILE, gate_tile, 0)

        @pl.when(t > 0)
        def _():
            finish_pair(t - 1)

        @pl.when(t < N_CHUNK - 1)
        def _():
            mlp_in(t + 1)

        @pl.when(t > 0)
        def _():
            zp_copy(t - 1).wait_send()

        def down_tile(n, c):
            cols = pl.ds(pl.multiple_of(n * N_TILE, N_TILE), N_TILE)
            own[half_rows(t), cols] = jnp.dot(h_buf[mine, :], wd[:, cols], preferred_element_type=F32).astype(BF16)
            pair_out[:, cols] = jnp.dot(h_buf[theirs, :], wd[:, cols], preferred_element_type=F32).astype(BF16)
            return c
        lax.fori_loop(0, 2560 // N_TILE, down_tile, 0)
        zp_copy(t).start()
        return carry
    lax.fori_loop(0, N_CHUNK, mlp_chunk, 0)
    finish_pair(N_CHUNK - 1)

    def result(j, dst, dst_base):
        t = 3 * chip + j
        zx_copy(j).wait_recv()

        def step(i, c):
            rows = sub_rows(t * HALF, i)
            proj = (own[rows, :].astype(F32) + z_in[sub_rows(j * HALF, i), :].astype(F32)).astype(BF16).astype(F32)
            final = res[rows, :].astype(F32) + rms(proj, gain4).astype(BF16).astype(F32)
            dst[sub_rows(dst_base, i), :] = final.astype(BF16)
            return c
        lax.fori_loop(0, HALF // SUB, step, 0)

    handover = remote(stage, out_ref.at[pl.ds(HALF, HALF)], out_ss, out_rs, mate)

    @pl.when(core == 0)
    def _():
        result(0, out_ref, 0)
        result(1, out_ref, 2 * HALF)
        result(2, stage, 0)
        handover.start()

    @pl.when(core == 1)
    def _():
        result(0, stage, 0)
        handover.start()
        result(1, out_ref, 0)
        result(2, out_ref, 2 * HALF)

    handover.wait()
    zp_copy(N_CHUNK - 1).wait_send()
    for t in range(N_CHUNK):
        yx_copy(t).wait_send()
    for j in range(3):
        zx_copy(3 * (1 - chip) + j).wait_send()


def run_layer(partial, cos_tab, sin_tab, q_pos, k_pos, w_query, w_key, w_value, w_out, w_gate, w_up, w_down, g1, g2, g3, g4):
    seq, dim = partial.shape
    vmem = pl.BlockSpec(memory_space=pltpu.VMEM)
    hbm = pl.BlockSpec(memory_space=pl.ANY)
    half_all = pltpu.VMEM((seq // 2, dim), BF16)
    dma = pltpu.SemaphoreType.DMA
    return pl.pallas_call(
        layer_kernel,
        name="layer",
        out_shape=jax.ShapeDtypeStruct((seq // 4, dim), BF16),
        in_specs=[hbm] + [vmem] * 4 + [hbm] * 7 + [vmem] * 4,
        out_specs=vmem,
        scratch_shapes=[
            pltpu.VMEM(w_query.shape, BF16), pltpu.VMEM(w_key.shape, BF16), pltpu.VMEM(w_value.shape, BF16),
            pltpu.VMEM(w_out.shape, BF16), pltpu.VMEM(w_gate.shape, BF16), pltpu.VMEM(w_up.shape, BF16),
            pltpu.VMEM(w_down.shape, BF16),
            half_all, half_all, half_all, half_all,
            pltpu.VMEM((2, ROWS, dim), BF16),
            pltpu.VMEM((seq, 256), BF16), pltpu.VMEM((seq, 256), BF16),
            pltpu.VMEM((ROWS, 512), BF16), pltpu.VMEM((ROWS, dim), BF16),
            pltpu.VMEM((HALF, dim), BF16), pltpu.VMEM((2, HALF, dim), BF16),
            pltpu.VMEM((3 * HALF, dim), BF16), pltpu.VMEM((HALF, dim), BF16),
            dma((7,)), dma((N_CHUNK,)), dma((N_CHUNK,)), dma((N_CHUNK,)), dma((N_CHUNK,)), dma((N_CHUNK,)),
            dma, dma, dma, dma,
            dma((N_CHUNK,)), dma((N_CHUNK,)), dma((2,)), dma((2,)), dma, dma((2,)),
            dma((3,)), dma((3,)), dma, dma,
        ],
        compiler_params=pltpu.CompilerParams(
            collective_id=0, has_side_effects=True, vmem_limit_bytes=67043328),
    )(partial, cos_tab, sin_tab, q_pos, k_pos, w_query, w_key, w_value, w_out, w_gate, w_up, w_down, g1, g2, g3, g4)


def solution(mesh):
    in_specs = (P("dp", None), P("dp", None), P("tp", None), P(None, "tp", None), P(None, "tp", None), P(None, "tp", None), P("tp", None, None), P(None, "tp"), P(None, "tp"), P("tp", None), P(None), P(None), P(None), P(None))

    def device_step(tokens, positions, embed_block, w_query, w_key, w_value, w_out, w_gate, w_up, w_down, g1, g2, g3, g4):
        dev_rank = lax.axis_index("tp")
        vocab_local, model_dim = embed_block.shape
        tokens, positions = tokens[0], positions[0]
        seq = tokens.shape[0]
        local_ids = tokens - dev_rank * vocab_local
        in_block = (local_ids >= 0) & (local_ids < vocab_local)
        looked = jnp.take(embed_block, jnp.clip(local_ids, 0, vocab_local - 1), axis=0)
        normalizer = jnp.sqrt(jnp.float32(model_dim)).astype(BF16)
        partial = jnp.where(in_block[:, None], looked * normalizer, jnp.zeros((), BF16))
        inv_freq = ROPE_BASE ** (-2.0 * jnp.arange(128, dtype=F32) / 256)
        angles = positions.astype(F32)[:, None] * inv_freq
        q_pos = jnp.broadcast_to(positions[:, None], (seq, 128))
        row = lambda gain: gain.reshape(1, model_dim)
        out = run_layer(
            partial, jnp.cos(angles), jnp.sin(angles), q_pos, positions.reshape(1, seq),
            w_query.reshape(model_dim, 512), w_key.reshape(model_dim, 256), w_value.reshape(model_dim, 256),
            w_out.reshape(512, model_dim), w_gate, w_up, w_down, row(g1), row(g2), row(g3), row(g4))
        return out[None]

    return jax.shard_map(device_step, mesh=mesh, in_specs=in_specs, out_specs=P("dp", "tp", None), check_vma=False)
```

```python
import functools

import jax
import jax.numpy as jnp
from jax import lax
from jax.experimental import pallas as pl
from jax.experimental.pallas import tpu as pltpu
from jax.sharding import PartitionSpec as P

WINDOW = 4096
QUERY_SCALE = 256.0 ** -0.5
SOFT_CAP = 50.0
NORM_EPS = 1e-6
ROPE_BASE = 10000.0

N_CHUNK = 6
ROWS = 128
HALF = 64
SUB = 16
N_TILE = 512
LEAD = 3
LAG = 2
LATE = 4
MESH = pl.DeviceIdType.MESH
F32 = jnp.float32
BF16 = jnp.bfloat16


def rms(block, gain):
    mean_sq = jnp.mean(block * block, axis=-1, keepdims=True)
    return block * lax.rsqrt(mean_sq + NORM_EPS) * gain


def layer_kernel(
    part_ref, cos_ref, sin_ref, kpos_ref,
    wq_hbm, wk_hbm, wv_hbm, wo_hbm, wg_hbm, wu_hbm, wd_hbm,
    g1_ref, g2_ref, g3_ref, g4_ref,
    out_ref,
    wq, wk, wv, wo, wg, wu, wd,
    own, sib, res, y_in, norm, k_all, v_all, o_buf, h_buf, y_out, y_pair, pair_out, pair_in, z_in, stage,
    w_sem, own_sem, sib_ss, sib_rs, ex_ss, ex_rs, a_ss, a_rs, yp_ss, yp_rs,
    yx_ss, yx_rs, m_ss, m_rs, zp_ss, zp_rs, zx_ss, zx_rs, out_ss, out_rs,
):
    dp = lax.axis_index("dp")
    tp = lax.axis_index("tp")
    chip = lax.div(tp, 2)
    core = lax.rem(tp, 2)
    mate = 2 * chip + 1 - core
    far = 2 * (1 - chip) + core

    def remote(src, dst, send_sem, recv_sem, target):
        return pltpu.make_async_remote_copy(
            src_ref=src, dst_ref=dst, send_sem=send_sem, recv_sem=recv_sem,
            device_id=(dp, target), device_id_type=MESH)

    def half_rows(t):
        return pl.ds(pl.multiple_of(t * HALF, HALF), HALF)

    mine = pl.ds(pl.multiple_of(core * HALF, HALF), HALF)

    def own_copy(t):
        rows = pl.ds(pl.multiple_of(t * ROWS + core * HALF, HALF), HALF)
        return pltpu.make_async_copy(part_ref.at[rows], own.at[half_rows(t)], own_sem.at[t])

    def sib_copy(t):
        rows = pl.ds(pl.multiple_of(t * ROWS + (1 - core) * HALF, HALF), HALF)
        return remote(part_ref.at[rows], sib.at[half_rows(t)], sib_ss.at[t], sib_rs.at[t], mate)

    def ex_copy(t):
        return remote(own.at[half_rows(t)], res.at[half_rows(t)], ex_ss.at[t], ex_rs.at[t], far)

    def norm_copy(slot, send_sem, recv_sem):
        return remote(norm.at[slot, mine], norm.at[slot, mine], send_sem, recv_sem, mate)

    def yp_copy():
        return remote(y_out, y_pair, yp_ss, yp_rs, mate)

    def yx_copy(t):
        return remote(sib.at[half_rows(t)], y_in.at[half_rows(t)], yx_ss.at[t], yx_rs.at[t], far)

    def m_copy(t):
        slot = lax.rem(t, 2)
        return norm_copy(slot, m_ss.at[slot], m_rs.at[slot])

    def zp_copy(t):
        slot = lax.rem(t, 2)
        return remote(pair_out, pair_in.at[slot], zp_ss, zp_rs.at[slot], mate)

    def zx_copy(t):
        j = lax.rem(t, 3)
        return remote(own.at[half_rows(t)], z_in.at[half_rows(j)], zx_ss.at[j], zx_rs.at[j], far)

    weights = [
        pltpu.make_async_copy(src, dst, w_sem.at[i])
        for i, (src, dst) in enumerate(
            [(wq_hbm, wq), (wk_hbm, wk), (wv_hbm, wv), (wo_hbm, wo), (wg_hbm, wg), (wu_hbm, wu), (wd_hbm, wd)])
    ]

    barrier = pltpu.get_barrier_semaphore()
    for peer in (mate, far):
        pl.semaphore_signal(barrier, inc=1, device_id=(dp, peer), device_id_type=MESH)
    pl.semaphore_wait(barrier, 2)

    for t in range(N_CHUNK):
        sib_copy(t).start()
        own_copy(t).start()
    for copy in weights:
        copy.start()

    def sub_rows(base, i):
        return pl.ds(pl.multiple_of(base + i * SUB, SUB), SUB)

    def combine(dst, other, dst_base, other_base):
        def step(i, carry):
            rows = sub_rows(dst_base, i)
            total = dst[rows, :].astype(F32) + other[sub_rows(other_base, i), :].astype(F32)
            dst[rows, :] = total.astype(BF16)
            return carry
        lax.fori_loop(0, HALF // SUB, step, 0)

    def send_embed(t, carry):
        own_copy(t).wait()
        sib_copy(t).wait_recv()
        combine(own, sib, t * HALF, t * HALF)

        @pl.when(t < LEAD)
        def _():
            ex_copy(t).start()
        return carry
    lax.fori_loop(0, N_CHUNK, send_embed, 0)

    k_all[...] = jnp.zeros_like(k_all)
    v_all[...] = jnp.zeros_like(v_all)
    gain1, gain2, gain3, gain4 = [(1.0 + g[...]).reshape(1, -1) for g in (g1_ref, g2_ref, g3_ref, g4_ref)]
    for t in range(N_CHUNK):
        sib_copy(t).wait_send()
    for copy in weights[:4]:
        copy.wait()

    def rope(states, cos_tab, sin_tab):
        lower, upper = states[:, :128], states[:, 128:]
        return lower * cos_tab - upper * sin_tab, upper * cos_tab + lower * sin_tab

    def split_halves(both):
        top, bottom = both[:HALF], both[HALF:]
        return jnp.where(core == 0, top, bottom), jnp.where(core == 0, bottom, top)

    def attention_chunk(t):
        base = t * HALF
        ex_copy(t).wait_recv()

        def embed_step(i, c):
            rows = sub_rows(base, i)
            embed = own[rows, :].astype(F32) + res[rows, :].astype(F32)
            res[rows, :] = embed.astype(BF16)
            norm[2, sub_rows(core * HALF, i), :] = rms(embed, gain1).astype(BF16)
            return c
        lax.fori_loop(0, HALF // SUB, embed_step, 0)

        copy = norm_copy(2, a_ss, a_rs)
        copy.start()
        copy.wait()
        act = norm[2]
        rows = pl.ds(pl.multiple_of(t * ROWS, ROWS), ROWS)
        cos_tab, sin_tab = cos_ref[rows, :], sin_ref[rows, :]
        lower, upper = rope(jnp.dot(act, wk[...], preferred_element_type=F32), cos_tab, sin_tab)
        k_all[rows, :128] = lower.astype(BF16)
        k_all[rows, 128:] = upper.astype(BF16)
        v_all[rows, :] = jnp.dot(act, wv[...], preferred_element_type=F32).astype(BF16)
        q_pos = jnp.broadcast_to(kpos_ref[:, rows], (8, ROWS)).T[:, :1]
        offset = q_pos - kpos_ref[...]
        keep = (offset >= 0) & (offset < WINDOW)
        for head in range(2):
            proj = jnp.dot(act, wq[:, head * 256:(head + 1) * 256], preferred_element_type=F32)
            lower, upper = rope(proj, cos_tab, sin_tab)
            query = jnp.concatenate([(lower * QUERY_SCALE).astype(BF16), (upper * QUERY_SCALE).astype(BF16)], axis=-1)
            scores = lax.dot_general(query, k_all[...], (((1,), (1,)), ((), ())), preferred_element_type=F32)
            weight = jnp.where(keep, jnp.exp(SOFT_CAP * jnp.tanh(scores * (1.0 / SOFT_CAP))), 0.0)
            weight = weight * (1.0 / jnp.sum(weight, axis=-1, keepdims=True))
            mixed = jnp.dot(weight.astype(BF16), v_all[...], preferred_element_type=F32)
            o_buf[:, head * 256:(head + 1) * 256] = mixed.astype(BF16)

        def out_tile(n, c):
            cols = pl.ds(pl.multiple_of(n * N_TILE, N_TILE), N_TILE)
            both = jnp.dot(o_buf[...], wo[:, cols], preferred_element_type=F32).astype(BF16)
            sib[half_rows(t), cols], y_out[:, cols] = split_halves(both)
            return c
        lax.fori_loop(0, 2560 // N_TILE, out_tile, 0, unroll=True)
        copy = yp_copy()
        copy.start()
        copy.wait()
        combine(sib, y_pair, base, 0)
        yx_copy(t).start()

        @pl.when(t + LEAD < N_CHUNK)
        def _():
            ex_copy(t + LEAD).start()

    def mlp_in(t):
        base = t * HALF
        slot = lax.rem(t, 2)
        yx_copy(t).wait_recv()

        def step(i, c):
            rows = sub_rows(base, i)
            proj = (sib[rows, :].astype(F32) + y_in[rows, :].astype(F32)).astype(BF16).astype(F32)
            resid = (res[rows, :].astype(F32) + rms(proj, gain2).astype(BF16).astype(F32)).astype(BF16)
            res[rows, :] = resid
            norm[slot, sub_rows(core * HALF, i), :] = rms(resid.astype(F32), gain3).astype(BF16)
            return c
        lax.fori_loop(0, HALF // SUB, step, 0)
        m_copy(t).start()

    def finish_pair(t):
        zp_copy(t).wait_recv()
        combine(own, pair_in.at[lax.rem(t, 2)], t * HALF, 0)

        @pl.when(lax.div(t, 3) != chip)
        def _():
            zx_copy(t).start()

    def mlp_chunk(t):
        slot = lax.rem(t, 2)

        @pl.when(t < LATE)
        def _():
            mlp_in(t)

        @pl.when(t == 0)
        def _():
            for copy in weights[4:]:
                copy.wait()
        ex_copy(t).wait_send()
        m_copy(t).wait()

        def gate_tile(n, c):
            cols = pl.ds(pl.multiple_of(n * N_TILE, N_TILE), N_TILE)
            gate = jnp.dot(norm[slot], wg[:, cols], preferred_element_type=F32)
            up = jnp.dot(norm[slot], wu[:, cols], preferred_element_type=F32)
            h_buf[:, cols] = (jax.nn.gelu(gate, approximate=True) * up).astype(BF16)
            return c
        lax.fori_loop(0, 2560 // N_TILE, gate_tile, 0, unroll=True)

        @pl.when(t > 0)
        def _():
            finish_pair(t - 1)

        @pl.when((t + 1 >= LATE) & (t < N_CHUNK - 1))
        def _():
            mlp_in(t + 1)

        @pl.when(t > 0)
        def _():
            zp_copy(t - 1).wait_send()

        def down_tile(n, c):
            cols = pl.ds(pl.multiple_of(n * N_TILE, N_TILE), N_TILE)
            both = jnp.dot(h_buf[...], wd[:, cols], preferred_element_type=F32).astype(BF16)
            own[half_rows(t), cols], pair_out[:, cols] = split_halves(both)
            return c
        lax.fori_loop(0, 2560 // N_TILE, down_tile, 0, unroll=True)
        zp_copy(t).start()

    def step(s, carry):
        @pl.when(s < N_CHUNK)
        def _():
            attention_chunk(s)

        @pl.when(s >= LAG)
        def _():
            mlp_chunk(s - LAG)
        return carry
    lax.fori_loop(0, N_CHUNK + LAG, step, 0)
    finish_pair(N_CHUNK - 1)

    def result(j, dst, dst_base):
        t = 3 * chip + j
        zx_copy(j).wait_recv()

        def step(i, c):
            rows = sub_rows(t * HALF, i)
            proj = (own[rows, :].astype(F32) + z_in[sub_rows(j * HALF, i), :].astype(F32)).astype(BF16).astype(F32)
            final = res[rows, :].astype(F32) + rms(proj, gain4).astype(BF16).astype(F32)
            dst[sub_rows(dst_base, i), :] = final.astype(BF16)
            return c
        lax.fori_loop(0, HALF // SUB, step, 0)

    handover = remote(stage, out_ref.at[pl.ds(HALF, HALF)], out_ss, out_rs, mate)

    @pl.when(core == 0)
    def _():
        result(0, out_ref, 0)
        result(1, out_ref, 2 * HALF)
        result(2, stage, 0)
        handover.start()

    @pl.when(core == 1)
    def _():
        result(0, stage, 0)
        handover.start()
        result(1, out_ref, 0)
        result(2, out_ref, 2 * HALF)

    handover.wait()
    zp_copy(N_CHUNK - 1).wait_send()
    for t in range(N_CHUNK):
        yx_copy(t).wait_send()
    for j in range(3):
        zx_copy(3 * (1 - chip) + j).wait_send()


def run_layer(partial, cos_tab, sin_tab, k_pos, w_query, w_key, w_value, w_out, w_gate, w_up, w_down, g1, g2, g3, g4):
    seq, dim = partial.shape
    vmem = pl.BlockSpec(memory_space=pltpu.VMEM)
    hbm = pl.BlockSpec(memory_space=pl.ANY)
    half_all = pltpu.VMEM((seq // 2, dim), BF16)
    dma = pltpu.SemaphoreType.DMA
    return pl.pallas_call(
        layer_kernel,
        name="layer",
        out_shape=jax.ShapeDtypeStruct((seq // 4, dim), BF16),
        in_specs=[hbm] + [vmem] * 3 + [hbm] * 7 + [vmem] * 4,
        out_specs=vmem,
        scratch_shapes=[
            pltpu.VMEM(w_query.shape, BF16), pltpu.VMEM(w_key.shape, BF16), pltpu.VMEM(w_value.shape, BF16),
            pltpu.VMEM(w_out.shape, BF16), pltpu.VMEM(w_gate.shape, BF16), pltpu.VMEM(w_up.shape, BF16),
            pltpu.VMEM(w_down.shape, BF16),
            half_all, half_all, half_all, half_all,
            pltpu.VMEM((3, ROWS, dim), BF16),
            pltpu.VMEM((seq, 256), BF16), pltpu.VMEM((seq, 256), BF16),
            pltpu.VMEM((ROWS, 512), BF16), pltpu.VMEM((ROWS, dim), BF16),
            pltpu.VMEM((HALF, dim), BF16), pltpu.VMEM((HALF, dim), BF16),
            pltpu.VMEM((HALF, dim), BF16), pltpu.VMEM((2, HALF, dim), BF16),
            pltpu.VMEM((3 * HALF, dim), BF16), pltpu.VMEM((HALF, dim), BF16),
            dma((7,)), dma((N_CHUNK,)), dma((N_CHUNK,)), dma((N_CHUNK,)), dma((N_CHUNK,)), dma((N_CHUNK,)),
            dma, dma, dma, dma,
            dma((N_CHUNK,)), dma((N_CHUNK,)), dma((2,)), dma((2,)), dma, dma((2,)),
            dma((3,)), dma((3,)), dma, dma,
        ],
        compiler_params=pltpu.CompilerParams(
            collective_id=0, has_side_effects=True, vmem_limit_bytes=67043328),
    )(partial, cos_tab, sin_tab, k_pos, w_query, w_key, w_value, w_out, w_gate, w_up, w_down, g1, g2, g3, g4)


def solution(mesh):
    in_specs = (P("dp", None), P("dp", None), P("tp", None), P(None, "tp", None), P(None, "tp", None), P(None, "tp", None), P("tp", None, None), P(None, "tp"), P(None, "tp"), P("tp", None), P(None), P(None), P(None), P(None))

    def device_step(tokens, positions, embed_block, w_query, w_key, w_value, w_out, w_gate, w_up, w_down, g1, g2, g3, g4):
        dev_rank = lax.axis_index("tp")
        vocab_local, model_dim = embed_block.shape
        tokens, positions = tokens[0], positions[0]
        seq = tokens.shape[0]
        local_ids = tokens - dev_rank * vocab_local
        in_block = (local_ids >= 0) & (local_ids < vocab_local)
        looked = embed_block.at[lax.rem(tokens, vocab_local)].get(mode='promise_in_bounds')
        normalizer = jnp.sqrt(jnp.float32(model_dim)).astype(BF16)
        partial = jnp.where(in_block[:, None], looked * normalizer, jnp.zeros((), BF16))
        inv_freq = ROPE_BASE ** (-2.0 * jnp.arange(128, dtype=F32) / 256)
        angles = positions.astype(F32)[:, None] * inv_freq
        out = run_layer(
            partial, jnp.cos(angles), jnp.sin(angles), positions.reshape(1, seq),
            w_query.reshape(model_dim, 512), w_key.reshape(model_dim, 256), w_value.reshape(model_dim, 256),
            w_out.reshape(512, model_dim), w_gate, w_up, w_down, g1, g2, g3, g4)
        return out[None]

    return jax.shard_map(device_step, mesh=mesh, in_specs=in_specs, out_specs=P("dp", "tp", None), check_vma=False)
```

```python
import functools

import jax
import jax.numpy as jnp
import numpy as np
from jax import lax
from jax.experimental import pallas as pl
from jax.experimental.pallas import tpu as pltpu
from jax.sharding import PartitionSpec as P

WINDOW = 4096
QUERY_SCALE = 256.0 ** -0.5
SOFT_CAP = 50.0
NORM_EPS = 1e-6
ROPE_BASE = 10000.0

N_CHUNK = 6
ROWS = 128
HALF = 64
SUB = 16
N_TILE = 512
WQ_ROWS = 320
LEAD = 3
LAG = 2
LATE = 4
MESH = pl.DeviceIdType.MESH
F32 = jnp.float32
BF16 = jnp.bfloat16


def rms(block, gain):
    mean_sq = jnp.mean(block * block, axis=-1, keepdims=True)
    return block * lax.rsqrt(mean_sq + NORM_EPS) * gain


def gather_kernel(scale, ids_ref, id_row_ref, table_ref, part_ref, groups, looked, in_sem, out_sem):
    block_rows = table_ref.shape[0]
    first = lax.axis_index("tp") * block_rows
    spread = 2 ** (block_rows.bit_length() - 1) - 1

    def start_block(b, carry):
        def start_eight(i, c):
            for u in range(8):
                place = b * ROWS + i * 8 + u
                token = ids_ref[0, place]
                local = token - first
                inside = (local >= 0) & (local < block_rows)
                row = jnp.where(inside, local, token & spread)
                group = pl.multiple_of(lax.shift_left(lax.shift_right_logical(row, 3), 3), 8)
                pltpu.make_async_copy(
                    table_ref.at[pl.ds(group, 8)], groups.at[pl.ds(pl.multiple_of(place * 8, 8), 8)], in_sem.at[b]).start()
            return c
        lax.fori_loop(0, ROWS // 8, start_eight, 0)
        return carry
    lax.fori_loop(0, N_CHUNK, start_block, 0)

    def out_copy(b):
        rows = pl.ds(pl.multiple_of(b * ROWS, ROWS), ROWS)
        return pltpu.make_async_copy(looked.at[rows], part_ref.at[rows], out_sem.at[b])

    def finish_block(b, carry):
        rows = pl.ds(pl.multiple_of(b * ROWS, ROWS), ROWS)
        fetched = pl.ds(pl.multiple_of(b * ROWS * 8, ROWS * 8), ROWS * 8)
        pltpu.make_async_copy(table_ref.at[pl.ds(0, ROWS * 8)], groups.at[fetched], in_sem.at[b]).wait()
        local = jnp.broadcast_to(id_row_ref[:, rows], (8, ROWS)).T[:, :1] - first
        inside = (local >= 0) & (local < block_rows)
        for h in range(2):
            half = slice(h * HALF, (h + 1) * HALF)
            place = lax.broadcasted_iota(jnp.int32, (HALF, 1), 0) * 8 + (local[half] & 7)
            target = jnp.where(inside[half], place, -1)
            pick = jnp.where(lax.broadcasted_iota(jnp.int32, (HALF, HALF * 8), 1) == target, 1.0, 0.0).astype(BF16)
            source = pl.ds(pl.multiple_of(b * ROWS * 8 + h * HALF * 8, HALF * 8), HALF * 8)
            dest = pl.ds(pl.multiple_of(b * ROWS + h * HALF, HALF), HALF)
            for n in range(2560 // N_TILE):
                cols = slice(n * N_TILE, (n + 1) * N_TILE)
                picked = jnp.dot(pick, groups[source, cols], preferred_element_type=F32)
                looked[dest, cols] = (picked * scale).astype(BF16)
        out_copy(b).start()
        return carry
    lax.fori_loop(0, N_CHUNK, finish_block, 0)
    for b in range(N_CHUNK):
        out_copy(b).wait()


def gather_rows(tokens, table):
    seq, dim = tokens.shape[1], table.shape[1]
    scale = float(np.sqrt(np.float32(dim)).astype(jnp.bfloat16))
    return pl.pallas_call(
        functools.partial(gather_kernel, scale),
        name="gather",
        out_shape=jax.ShapeDtypeStruct((seq, dim), BF16),
        in_specs=[pl.BlockSpec(memory_space=pltpu.SMEM), pl.BlockSpec(memory_space=pltpu.VMEM), pl.BlockSpec(memory_space=pl.ANY)],
        out_specs=pl.BlockSpec(memory_space=pl.ANY),
        scratch_shapes=[
            pltpu.VMEM((seq * 8, dim), BF16), pltpu.VMEM((seq, dim), BF16),
            pltpu.SemaphoreType.DMA((N_CHUNK,)), pltpu.SemaphoreType.DMA((N_CHUNK,)),
        ],
        compiler_params=pltpu.CompilerParams(vmem_limit_bytes=56 * 2 ** 20),
    )(tokens, tokens, table)


def layer_kernel(
    part_ref, kpos_ref, freq_ref,
    wq_hbm, wk_hbm, wv_hbm, wo_hbm, wg_hbm, wu_hbm, wd_hbm,
    g1_ref, g2_ref, g3_ref, g4_ref,
    out_ref,
    wq, wk, wv, wo, wg, wu, wd,
    wq_in, cos_tabs, sin_tabs, own, sib, res, y_in, norm, k_all, v_all, o_buf, h_buf, y_out, y_pair, pair_out, pair_in, z_in, stage,
    wq_sem, w_sem, own_sem, sib_ss, sib_rs, ex_ss, ex_rs, a_ss, a_rs, yp_ss, yp_rs,
    yx_ss, yx_rs, m_ss, m_rs, zp_ss, zp_rs, zx_ss, zx_rs, out_ss, out_rs,
):
    dp = lax.axis_index("dp")
    tp = lax.axis_index("tp")
    chip = lax.div(tp, 2)
    core = lax.rem(tp, 2)
    mate = 2 * chip + 1 - core
    far = 2 * (1 - chip) + core

    def remote(src, dst, send_sem, recv_sem, target):
        return pltpu.make_async_remote_copy(
            src_ref=src, dst_ref=dst, send_sem=send_sem, recv_sem=recv_sem,
            device_id=(dp, target), device_id_type=MESH)

    def half_rows(t):
        return pl.ds(pl.multiple_of(t * HALF, HALF), HALF)

    mine = pl.ds(pl.multiple_of(core * HALF, HALF), HALF)

    def own_copy(t):
        rows = pl.ds(pl.multiple_of(t * ROWS + core * HALF, HALF), HALF)
        return pltpu.make_async_copy(part_ref.at[rows], own.at[half_rows(t)], own_sem.at[t])

    def sib_copy(t):
        rows = pl.ds(pl.multiple_of(t * ROWS + (1 - core) * HALF, HALF), HALF)
        return remote(part_ref.at[rows], sib.at[half_rows(t)], sib_ss.at[t], sib_rs.at[t], mate)

    def ex_copy(t):
        return remote(own.at[half_rows(t)], res.at[half_rows(t)], ex_ss.at[t], ex_rs.at[t], far)

    def norm_copy(slot, send_sem, recv_sem):
        return remote(norm.at[slot, mine], norm.at[slot, mine], send_sem, recv_sem, mate)

    def yp_copy():
        return remote(y_out, y_pair, yp_ss, yp_rs, mate)

    def yx_copy(t):
        return remote(sib.at[half_rows(t)], y_in.at[half_rows(t)], yx_ss.at[t], yx_rs.at[t], far)

    def m_copy(t):
        slot = lax.rem(t, 2)
        return norm_copy(slot, m_ss.at[slot], m_rs.at[slot])

    def zp_copy(t):
        slot = lax.rem(t, 2)
        return remote(pair_out, pair_in.at[slot], zp_ss, zp_rs.at[slot], mate)

    def zx_copy(t):
        j = lax.rem(t, 3)
        return remote(own.at[half_rows(t)], z_in.at[half_rows(j)], zx_ss.at[j], zx_rs.at[j], far)

    weights = [
        pltpu.make_async_copy(src, dst, w_sem.at[i])
        for i, (src, dst) in enumerate(
            [(wk_hbm, wk), (wv_hbm, wv), (wo_hbm, wo), (wg_hbm, wg), (wu_hbm, wu), (wd_hbm, wd)])
    ]

    barrier = pltpu.get_barrier_semaphore()
    for peer in (mate, far):
        pl.semaphore_signal(barrier, inc=1, device_id=(dp, peer), device_id_type=MESH)
    pl.semaphore_wait(barrier, 2)

    for t in range(N_CHUNK):
        sib_copy(t).start()
        own_copy(t).start()

    def wq_copy(i):
        slot = lax.rem(i, 2)
        rows = pl.ds(pl.multiple_of(i * WQ_ROWS, WQ_ROWS), WQ_ROWS)
        return pltpu.make_async_copy(wq_hbm.at[rows], wq_in.at[slot], wq_sem.at[slot])

    wq_copy(0).start()
    wq_copy(1).start()
    for copy in weights:
        copy.start()

    def sub_rows(base, i):
        return pl.ds(pl.multiple_of(base + i * SUB, SUB), SUB)

    def combine(dst, other, dst_base, other_base):
        def step(i, carry):
            rows = sub_rows(dst_base, i)
            total = dst[rows, :].astype(F32) + other[sub_rows(other_base, i), :].astype(F32)
            dst[rows, :] = total.astype(BF16)
            return carry
        lax.fori_loop(0, HALF // SUB, step, 0)

    def send_embed(t, carry):
        own_copy(t).wait()
        sib_copy(t).wait_recv()
        combine(own, sib, t * HALF, t * HALF)

        @pl.when(t < LEAD)
        def _():
            ex_copy(t).start()
        return carry
    lax.fori_loop(0, N_CHUNK, send_embed, 0)

    k_all[...] = jnp.zeros_like(k_all)
    v_all[...] = jnp.zeros_like(v_all)
    gain1, gain2, gain3, gain4 = [(1.0 + g[...]).reshape(1, -1) for g in (g1_ref, g2_ref, g3_ref, g4_ref)]

    def chunk_positions(rows):
        return jnp.broadcast_to(kpos_ref[:, rows], (8, ROWS)).T[:, :1]

    def tables(t, carry):
        rows = pl.ds(pl.multiple_of(t * ROWS, ROWS), ROWS)
        angles = chunk_positions(rows).astype(F32) * freq_ref[...]
        cos_tabs[rows, :] = jnp.cos(angles)
        sin_tabs[rows, :] = jnp.sin(angles)
        return carry
    lax.fori_loop(0, N_CHUNK, tables, 0)

    def spread_wq(i, carry):
        slot = lax.rem(i, 2)
        wq_copy(i).wait()
        for r in range(0, WQ_ROWS, 64):
            rows = pl.ds(pl.multiple_of(i * WQ_ROWS + r, 64), 64)
            for head in range(2):
                wq[rows, head * 256:(head + 1) * 256] = wq_in[slot, r:r + 64, head, :]

        @pl.when(i + 2 < 2560 // WQ_ROWS)
        def _():
            wq_copy(i + 2).start()
        return carry
    lax.fori_loop(0, 2560 // WQ_ROWS, spread_wq, 0)
    for t in range(N_CHUNK):
        sib_copy(t).wait_send()
    for copy in weights[:3]:
        copy.wait()

    def rope(states, cos_tab, sin_tab):
        lower, upper = states[:, :128], states[:, 128:]
        return lower * cos_tab - upper * sin_tab, upper * cos_tab + lower * sin_tab

    def split_halves(both):
        top, bottom = both[:HALF], both[HALF:]
        return jnp.where(core == 0, top, bottom), jnp.where(core == 0, bottom, top)

    def attention_chunk(t):
        base = t * HALF
        ex_copy(t).wait_recv()

        def embed_step(i, c):
            rows = sub_rows(base, i)
            embed = own[rows, :].astype(F32) + res[rows, :].astype(F32)
            res[rows, :] = embed.astype(BF16)
            norm[2, sub_rows(core * HALF, i), :] = rms(embed, gain1).astype(BF16)
            return c
        lax.fori_loop(0, HALF // SUB, embed_step, 0)

        copy = norm_copy(2, a_ss, a_rs)
        copy.start()
        copy.wait()
        act = norm[2]
        rows = pl.ds(pl.multiple_of(t * ROWS, ROWS), ROWS)
        cos_tab, sin_tab = cos_tabs[rows, :], sin_tabs[rows, :]
        lower, upper = rope(jnp.dot(act, wk[...], preferred_element_type=F32), cos_tab, sin_tab)
        k_all[rows, :128] = lower.astype(BF16)
        k_all[rows, 128:] = upper.astype(BF16)
        v_all[rows, :] = jnp.dot(act, wv[...], preferred_element_type=F32).astype(BF16)
        offset = chunk_positions(rows) - kpos_ref[...]
        keep = (offset >= 0) & (offset < WINDOW)
        for head in range(2):
            proj = jnp.dot(act, wq[:, head * 256:(head + 1) * 256], preferred_element_type=F32)
            lower, upper = rope(proj, cos_tab, sin_tab)
            query = jnp.concatenate([(lower * QUERY_SCALE).astype(BF16), (upper * QUERY_SCALE).astype(BF16)], axis=-1)
            scores = lax.dot_general(query, k_all[...], (((1,), (1,)), ((), ())), preferred_element_type=F32)
            weight = jnp.where(keep, jnp.exp(SOFT_CAP * jnp.tanh(scores * (1.0 / SOFT_CAP))), 0.0)
            weight = weight * (1.0 / jnp.sum(weight, axis=-1, keepdims=True))
            mixed = jnp.dot(weight.astype(BF16), v_all[...], preferred_element_type=F32)
            o_buf[:, head * 256:(head + 1) * 256] = mixed.astype(BF16)

        def out_tile(n, c):
            cols = pl.ds(pl.multiple_of(n * N_TILE, N_TILE), N_TILE)
            both = jnp.dot(o_buf[...], wo[:, cols], preferred_element_type=F32).astype(BF16)
            sib[half_rows(t), cols], y_out[:, cols] = split_halves(both)
            return c
        lax.fori_loop(0, 2560 // N_TILE, out_tile, 0, unroll=True)
        copy = yp_copy()
        copy.start()
        copy.wait()
        combine(sib, y_pair, base, 0)
        yx_copy(t).start()

        @pl.when(t + LEAD < N_CHUNK)
        def _():
            ex_copy(t + LEAD).start()

    def mlp_in(t):
        base = t * HALF
        slot = lax.rem(t, 2)
        yx_copy(t).wait_recv()

        def step(i, c):
            rows = sub_rows(base, i)
            proj = (sib[rows, :].astype(F32) + y_in[rows, :].astype(F32)).astype(BF16).astype(F32)
            resid = (res[rows, :].astype(F32) + rms(proj, gain2).astype(BF16).astype(F32)).astype(BF16)
            res[rows, :] = resid
            norm[slot, sub_rows(core * HALF, i), :] = rms(resid.astype(F32), gain3).astype(BF16)
            return c
        lax.fori_loop(0, HALF // SUB, step, 0)
        m_copy(t).start()

    def finish_pair(t):
        zp_copy(t).wait_recv()
        combine(own, pair_in.at[lax.rem(t, 2)], t * HALF, 0)

        @pl.when((lax.div(t, 3) != chip) & (t >= LAG))
        def _():
            zx_copy(t).start()

    def mlp_chunk(t):
        slot = lax.rem(t, 2)

        @pl.when(t < LATE)
        def _():
            mlp_in(t)

        @pl.when(t == 0)
        def _():
            for copy in weights[3:]:
                copy.wait()
        ex_copy(t).wait_send()
        m_copy(t).wait()

        def gate_tile(n, c):
            cols = pl.ds(pl.multiple_of(n * N_TILE, N_TILE), N_TILE)
            gate = jnp.dot(norm[slot], wg[:, cols], preferred_element_type=F32)
            up = jnp.dot(norm[slot], wu[:, cols], preferred_element_type=F32)
            h_buf[:, cols] = (jax.nn.gelu(gate, approximate=True) * up).astype(BF16)
            return c
        lax.fori_loop(0, 2560 // N_TILE, gate_tile, 0, unroll=True)

        @pl.when(t > 0)
        def _():
            finish_pair(t - 1)

        @pl.when((t + 1 >= LATE) & (t < N_CHUNK - 1))
        def _():
            mlp_in(t + 1)

        @pl.when(t > 0)
        def _():
            zp_copy(t - 1).wait_send()

        def down_tile(n, c):
            cols = pl.ds(pl.multiple_of(n * N_TILE, N_TILE), N_TILE)
            both = jnp.dot(h_buf[...], wd[:, cols], preferred_element_type=F32).astype(BF16)
            own[half_rows(t), cols], pair_out[:, cols] = split_halves(both)
            return c
        lax.fori_loop(0, 2560 // N_TILE, down_tile, 0, unroll=True)
        zp_copy(t).start()

    def step(s, carry):
        @pl.when(s < N_CHUNK)
        def _():
            attention_chunk(s)

        @pl.when((s == N_CHUNK - 1) & (chip != 0))
        def _():
            for t in range(LAG):
                zx_copy(t).start()

        @pl.when(s >= LAG)
        def _():
            mlp_chunk(s - LAG)
        return carry
    lax.fori_loop(0, N_CHUNK + LAG, step, 0)
    finish_pair(N_CHUNK - 1)

    def result(j, dst, dst_base):
        t = 3 * chip + j
        zx_copy(j).wait_recv()

        def step(i, c):
            rows = sub_rows(t * HALF, i)
            proj = (own[rows, :].astype(F32) + z_in[sub_rows(j * HALF, i), :].astype(F32)).astype(BF16).astype(F32)
            final = res[rows, :].astype(F32) + rms(proj, gain4).astype(BF16).astype(F32)
            dst[sub_rows(dst_base, i), :] = final.astype(BF16)
            return c
        lax.fori_loop(0, HALF // SUB, step, 0)

    handover = remote(stage, out_ref.at[pl.ds(HALF, HALF)], out_ss, out_rs, mate)

    @pl.when(core == 0)
    def _():
        result(0, out_ref, 0)
        result(1, out_ref, 2 * HALF)
        result(2, stage, 0)
        handover.start()

    @pl.when(core == 1)
    def _():
        result(0, stage, 0)
        handover.start()
        result(1, out_ref, 0)
        result(2, out_ref, 2 * HALF)

    handover.wait()
    zp_copy(N_CHUNK - 1).wait_send()
    for t in range(N_CHUNK):
        yx_copy(t).wait_send()
    for j in range(3):
        zx_copy(3 * (1 - chip) + j).wait_send()


def run_layer(partial, k_pos, inv_freq, w_query, w_key, w_value, w_out, w_gate, w_up, w_down, g1, g2, g3, g4):
    seq, dim = partial.shape
    vmem = pl.BlockSpec(memory_space=pltpu.VMEM)
    hbm = pl.BlockSpec(memory_space=pl.ANY)
    half_all = pltpu.VMEM((seq // 2, dim), BF16)
    dma = pltpu.SemaphoreType.DMA
    return pl.pallas_call(
        layer_kernel,
        name="layer",
        out_shape=jax.ShapeDtypeStruct((seq // 4, dim), BF16),
        in_specs=[hbm] + [vmem] * 2 + [hbm] * 7 + [vmem] * 4,
        out_specs=vmem,
        scratch_shapes=[
            pltpu.VMEM((dim, 512), BF16), pltpu.VMEM(w_key.shape, BF16), pltpu.VMEM(w_value.shape, BF16),
            pltpu.VMEM(w_out.shape, BF16), pltpu.VMEM(w_gate.shape, BF16), pltpu.VMEM(w_up.shape, BF16),
            pltpu.VMEM(w_down.shape, BF16),
            pltpu.VMEM((2, WQ_ROWS, 2, 256), BF16), pltpu.VMEM((seq, 128), F32), pltpu.VMEM((seq, 128), F32),
            half_all, half_all, half_all, half_all,
            pltpu.VMEM((3, ROWS, dim), BF16),
            pltpu.VMEM((seq, 256), BF16), pltpu.VMEM((seq, 256), BF16),
            pltpu.VMEM((ROWS, 512), BF16), pltpu.VMEM((ROWS, dim), BF16),
            pltpu.VMEM((HALF, dim), BF16), pltpu.VMEM((HALF, dim), BF16),
            pltpu.VMEM((HALF, dim), BF16), pltpu.VMEM((2, HALF, dim), BF16),
            pltpu.VMEM((3 * HALF, dim), BF16), pltpu.VMEM((HALF, dim), BF16),
            dma((2,)), dma((6,)), dma((N_CHUNK,)), dma((N_CHUNK,)), dma((N_CHUNK,)), dma((N_CHUNK,)), dma((N_CHUNK,)),
            dma, dma, dma, dma,
            dma((N_CHUNK,)), dma((N_CHUNK,)), dma((2,)), dma((2,)), dma, dma((2,)),
            dma((3,)), dma((3,)), dma, dma,
        ],
        compiler_params=pltpu.CompilerParams(
            collective_id=0, has_side_effects=True, vmem_limit_bytes=67043328),
    )(partial, k_pos, inv_freq, w_query, w_key, w_value, w_out, w_gate, w_up, w_down, g1, g2, g3, g4)


def solution(mesh):
    in_specs = (P("dp", None), P("dp", None), P("tp", None), P(None, "tp", None), P(None, "tp", None), P(None, "tp", None), P("tp", None, None), P(None, "tp"), P(None, "tp"), P("tp", None), P(None), P(None), P(None), P(None))

    def device_step(tokens, positions, embed_block, w_query, w_key, w_value, w_out, w_gate, w_up, w_down, g1, g2, g3, g4):
        model_dim = embed_block.shape[1]
        partial = gather_rows(tokens, embed_block)
        inv_freq = (ROPE_BASE ** (-2.0 * np.arange(128) / 256)).astype(np.float32).reshape(1, 128)
        out = run_layer(
            partial, positions, jnp.asarray(inv_freq),
            w_query, w_key.reshape(model_dim, 256), w_value.reshape(model_dim, 256),
            w_out.reshape(512, model_dim), w_gate, w_up, w_down, g1, g2, g3, g4)
        return out[None]

    return jax.shard_map(device_step, mesh=mesh, in_specs=in_specs, out_specs=P("dp", "tp", None), check_vma=False)
```

```python
import functools

import jax
import jax.numpy as jnp
import numpy as np
from jax import lax
from jax.experimental import pallas as pl
from jax.experimental.pallas import tpu as pltpu
from jax.sharding import PartitionSpec as P

WINDOW = 4096
QUERY_SCALE = 256.0 ** -0.5
SOFT_CAP = 50.0
NORM_EPS = 1e-6
ROPE_BASE = 10000.0

N_CHUNK = 6
ROWS = 128
HALF = 64
SUB = 16
N_TILE = 512
WQ_ROWS = 256
LEAD = 3
LAG = 2
LATE = 4
MESH = pl.DeviceIdType.MESH
F32 = jnp.float32
BF16 = jnp.bfloat16


def rms(block, gain):
    mean_sq = jnp.mean(block * block, axis=-1, keepdims=True)
    return block * lax.rsqrt(mean_sq + NORM_EPS) * gain


def layer_kernel(
    block_rows, scale,
    rows_ref, ids_ref, kpos_ref, freq_ref,
    wq_hbm, wk_hbm, wv_hbm, wo_hbm, wg_hbm, wu_hbm, wd_hbm,
    g1_ref, g2_ref, g3_ref, g4_ref,
    out_ref,
    wqkv, wo, wg, wu, wd,
    wq_in, own, sib, res, y_in, norm, k_all, v_all, o_buf, h_buf, y_out, y_pair, pair_out, pair_in, z_in, stage,
    wq_sem, w_sem, own_sem, sib_ss, sib_rs, ex_ss, ex_rs, a_ss, a_rs, yp_ss, yp_rs,
    yx_ss, yx_rs, m_ss, m_rs, zp_ss, zp_rs, zx_ss, zx_rs, out_ss, out_rs, keep_sem,
):
    dp = lax.axis_index("dp")
    tp = lax.axis_index("tp")
    chip = lax.div(tp, 2)
    core = lax.rem(tp, 2)
    mate = 2 * chip + 1 - core
    far = 2 * (1 - chip) + core

    def remote(src, dst, send_sem, recv_sem, target):
        return pltpu.make_async_remote_copy(
            src_ref=src, dst_ref=dst, send_sem=send_sem, recv_sem=recv_sem,
            device_id=(dp, target), device_id_type=MESH)

    def half_rows(t):
        return pl.ds(pl.multiple_of(t * HALF, HALF), HALF)

    mine = pl.ds(pl.multiple_of(core * HALF, HALF), HALF)

    def own_copy(t):
        rows = pl.ds(pl.multiple_of(t * ROWS + core * HALF, HALF), HALF)
        return pltpu.make_async_copy(rows_ref.at[rows], own.at[half_rows(t)], own_sem.at[t])

    def sib_copy(t):
        rows = pl.ds(pl.multiple_of(t * ROWS + (1 - core) * HALF, HALF), HALF)
        return remote(rows_ref.at[rows], sib.at[half_rows(t)], sib_ss.at[t], sib_rs.at[t], mate)

    def ex_copy(t):
        return remote(own.at[half_rows(t)], res.at[half_rows(t)], ex_ss.at[t], ex_rs.at[t], far)

    def norm_copy(slot, send_sem, recv_sem):
        return remote(norm.at[slot, mine], norm.at[slot, mine], send_sem, recv_sem, mate)

    def yp_copy():
        return remote(y_out, y_pair, yp_ss, yp_rs, mate)

    def yx_copy(t):
        return remote(sib.at[half_rows(t)], y_in.at[half_rows(t)], yx_ss.at[t], yx_rs.at[t], far)

    def m_copy(t):
        slot = lax.rem(t, 2)
        return norm_copy(slot, m_ss.at[slot], m_rs.at[slot])

    def zp_copy(t):
        slot = lax.rem(t, 2)
        return remote(pair_out, pair_in.at[slot], zp_ss, zp_rs.at[slot], mate)

    def zx_copy(t):
        j = lax.rem(t, 3)
        return remote(own.at[half_rows(t)], z_in.at[half_rows(j)], zx_ss.at[j], zx_rs.at[j], far)

    weights = [
        pltpu.make_async_copy(src, dst, w_sem.at[i])
        for i, (src, dst) in enumerate(
            [(wk_hbm, wqkv.at[:, pl.ds(512, 256)]), (wv_hbm, wqkv.at[:, pl.ds(768, 256)]), (wo_hbm, wo), (wg_hbm, wg), (wu_hbm, wu), (wd_hbm, wd)])
    ]

    barrier = pltpu.get_barrier_semaphore()
    for peer in (mate, far):
        pl.semaphore_signal(barrier, inc=1, device_id=(dp, peer), device_id_type=MESH)
    pl.semaphore_wait(barrier, 2)

    for t in range(N_CHUNK):
        sib_copy(t).start()
        own_copy(t).start()

    def wq_copy(i):
        slot = lax.rem(i, 2)
        rows = pl.ds(pl.multiple_of(i * WQ_ROWS, WQ_ROWS), WQ_ROWS)
        return pltpu.make_async_copy(wq_hbm.at[rows], wq_in.at[slot], wq_sem.at[slot])

    wq_copy(0).start()
    wq_copy(1).start()
    for copy in weights:
        copy.start()

    def sub_rows(base, i):
        return pl.ds(pl.multiple_of(base + i * SUB, SUB), SUB)

    def combine(dst, other, dst_base, other_base):
        def step(i, carry):
            rows = sub_rows(dst_base, i)
            total = dst[rows, :].astype(F32) + other[sub_rows(other_base, i), :].astype(F32)
            dst[rows, :] = total.astype(BF16)
            return carry
        lax.fori_loop(0, HALF // SUB, step, 0)

    def column(row_ref, t):
        rows = pl.ds(pl.multiple_of(t * ROWS, ROWS), ROWS)
        return jnp.broadcast_to(row_ref[:, rows], (8, ROWS)).T[:, :1]

    def send_embed(t, carry):
        own_copy(t).wait()
        sib_copy(t).wait_recv()
        ids = column(ids_ref, t)
        ids = jnp.where(core == 0, ids[:HALF], ids[HALF:])
        local, local_mate = ids - tp * block_rows, ids - mate * block_rows
        held = (local >= 0) & (local < block_rows)
        held_mate = (local_mate >= 0) & (local_mate < block_rows)
        for r in range(0, HALF, SUB):
            part = slice(r, r + SUB)
            rows = pl.ds(pl.multiple_of(t * HALF + r, SUB), SUB)
            looked = jnp.where(held[part], own[rows, :].astype(F32), jnp.where(held_mate[part], sib[rows, :].astype(F32), 0.0))
            own[rows, :] = (looked * scale).astype(BF16)

        @pl.when(t < LEAD)
        def _():
            ex_copy(t).start()
        return carry
    lax.fori_loop(0, N_CHUNK, send_embed, 0)

    k_all[...] = jnp.zeros_like(k_all)
    v_all[...] = jnp.zeros_like(v_all)
    gain1, gain2, gain3, gain4 = [(1.0 + g[...]).reshape(1, -1) for g in (g1_ref, g2_ref, g3_ref, g4_ref)]

    out_row = lax.broadcasted_iota(jnp.int32, (256, 256), 0)
    in_row = lax.broadcasted_iota(jnp.int32, (256, 256), 1)
    split_heads = jnp.where(in_row == jnp.where(out_row < 128, 2 * out_row, 2 * out_row - 255), 1.0, 0.0).astype(BF16)

    def spread_wq(i, carry):
        slot = lax.rem(i, 2)
        wq_copy(i).wait()
        for r in range(0, WQ_ROWS, 128):
            rows = pl.ds(pl.multiple_of(i * WQ_ROWS + r, 128), 128)
            both = wq_in[slot, r:r + 128].reshape(256, 256)
            both = jnp.dot(split_heads, both, preferred_element_type=F32).astype(BF16)
            wqkv[rows, :256] = both[:128]
            wqkv[rows, 256:512] = both[128:]

        @pl.when(i + 2 < 2560 // WQ_ROWS)
        def _():
            wq_copy(i + 2).start()
        return carry
    lax.fori_loop(0, 2560 // WQ_ROWS, spread_wq, 0)
    for t in range(N_CHUNK):
        sib_copy(t).wait_send()
    for copy in weights[:3]:
        copy.wait()

    def rope(states, cos_tab, sin_tab):
        lower, upper = states[:, :128], states[:, 128:]
        return lower * cos_tab - upper * sin_tab, upper * cos_tab + lower * sin_tab

    def split_halves(both):
        top, bottom = both[:HALF], both[HALF:]
        return jnp.where(core == 0, top, bottom), jnp.where(core == 0, bottom, top)

    def a_copy(t):
        slot = lax.rem(t, 2)
        return norm_copy(2 + slot, a_ss.at[slot], a_rs.at[slot])

    def embed_in(t):
        base = t * HALF
        slot = 2 + lax.rem(t, 2)
        ex_copy(t).wait_recv()

        def embed_step(i, c):
            rows = sub_rows(base, i)
            embed = own[rows, :].astype(F32) + res[rows, :].astype(F32)
            res[rows, :] = embed.astype(BF16)
            norm[slot, sub_rows(core * HALF, i), :] = rms(embed, gain1).astype(BF16)
            return c
        lax.fori_loop(0, HALF // SUB, embed_step, 0)
        a_copy(t).start()

    def attention_chunk(t):
        slot = 2 + lax.rem(t, 2)
        rows = pl.ds(pl.multiple_of(t * ROWS, ROWS), ROWS)

        @pl.when(t <= LAG)
        def _():
            embed_in(t)
        q_pos = column(kpos_ref, t)
        angles = q_pos.astype(F32) * freq_ref[...]
        cos_tab, sin_tab = jnp.cos(angles), jnp.sin(angles)
        offset = q_pos - kpos_ref[...]
        keep = (offset >= 0) & (offset < WINDOW)
        a_copy(t).wait()
        proj = jnp.dot(norm[slot], wqkv[:, 512:], preferred_element_type=F32)
        lower, upper = rope(proj[:, :256], cos_tab, sin_tab)
        k_all[rows, :128] = lower.astype(BF16)
        k_all[rows, 128:] = upper.astype(BF16)
        v_all[rows, :] = proj[:, 256:].astype(BF16)
        proj = jnp.dot(norm[slot], wqkv[:, :512], preferred_element_type=F32)
        for head in range(2):
            lower, upper = rope(proj[:, head * 256:(head + 1) * 256], cos_tab, sin_tab)
            query = jnp.concatenate([(lower * QUERY_SCALE).astype(BF16), (upper * QUERY_SCALE).astype(BF16)], axis=-1)
            scores = lax.dot_general(query, k_all[...], (((1,), (1,)), ((), ())), preferred_element_type=F32)
            weight = jnp.where(keep, jnp.exp(SOFT_CAP * jnp.tanh(scores * (1.0 / SOFT_CAP))), 0.0)
            weight = weight * (1.0 / jnp.sum(weight, axis=-1, keepdims=True))
            mixed = jnp.dot(weight.astype(BF16), v_all[...], preferred_element_type=F32)
            o_buf[:, head * 256:(head + 1) * 256] = mixed.astype(BF16)

        def out_tile(n, c):
            cols = pl.ds(pl.multiple_of(n * N_TILE, N_TILE), N_TILE)
            both = jnp.dot(o_buf[...], wo[:, cols], preferred_element_type=F32).astype(BF16)
            sib[half_rows(t), cols], y_out[:, cols] = split_halves(both)
            return c
        lax.fori_loop(0, 2560 // N_TILE, out_tile, 0, unroll=True)
        yp_copy().start()

    def send_proj(t):
        yp_copy().wait()
        combine(sib, y_pair, t * HALF, 0)
        yx_copy(t).start()

        @pl.when(t + LEAD < N_CHUNK)
        def _():
            ex_copy(t + LEAD).start()

    def mlp_in(t):
        base = t * HALF
        slot = lax.rem(t, 2)
        yx_copy(t).wait_recv()

        def step(i, c):
            rows = sub_rows(base, i)
            proj = (sib[rows, :].astype(F32) + y_in[rows, :].astype(F32)).astype(BF16).astype(F32)
            resid = (res[rows, :].astype(F32) + rms(proj, gain2).astype(BF16).astype(F32)).astype(BF16)
            res[rows, :] = resid
            norm[slot, sub_rows(core * HALF, i), :] = rms(resid.astype(F32), gain3).astype(BF16)
            return c
        lax.fori_loop(0, HALF // SUB, step, 0)
        m_copy(t).start()

    def finish_pair(t):
        zp_copy(t).wait_recv()
        combine(own, pair_in.at[lax.rem(t, 2)], t * HALF, 0)

        @pl.when((lax.div(t, 3) != chip) & (t >= LAG))
        def _():
            zx_copy(t).start()

    def mlp_chunk(t):
        slot = lax.rem(t, 2)

        @pl.when(t == 0)
        def _():
            for copy in weights[3:]:
                copy.wait()
        ex_copy(t).wait_send()
        m_copy(t).wait()

        def gate_tile(n, c):
            cols = pl.ds(pl.multiple_of(n * N_TILE, N_TILE), N_TILE)
            gate = jnp.dot(norm[slot], wg[:, cols], preferred_element_type=F32)
            up = jnp.dot(norm[slot], wu[:, cols], preferred_element_type=F32)
            h_buf[:, cols] = (jax.nn.gelu(gate, approximate=True) * up).astype(BF16)
            return c
        lax.fori_loop(0, 2560 // N_TILE, gate_tile, 0, unroll=True)

        @pl.when(t > 0)
        def _():
            finish_pair(t - 1)

        @pl.when(t + LAG + 1 < N_CHUNK)
        def _():
            embed_in(t + LAG + 1)

        @pl.when((t + 1 >= LATE) & (t < N_CHUNK - 1))
        def _():
            mlp_in(t + 1)

        @pl.when(t > 0)
        def _():
            zp_copy(t - 1).wait_send()

        def down_tile(n, c):
            cols = pl.ds(pl.multiple_of(n * N_TILE, N_TILE), N_TILE)
            both = jnp.dot(h_buf[...], wd[:, cols], preferred_element_type=F32).astype(BF16)
            own[half_rows(t), cols], pair_out[:, cols] = split_halves(both)
            return c
        lax.fori_loop(0, 2560 // N_TILE, down_tile, 0, unroll=True)
        zp_copy(t).start()

    def step(s, carry):
        @pl.when(s < N_CHUNK)
        def _():
            attention_chunk(s)

        @pl.when((s >= LAG) & (s < LATE + LAG))
        def _():
            mlp_in(s - LAG)

        @pl.when(s < N_CHUNK)
        def _():
            send_proj(s)

        @pl.when((s == N_CHUNK - 1) & (chip != 0))
        def _():
            for t in range(LAG):
                zx_copy(t).start()

        @pl.when(s >= LAG)
        def _():
            mlp_chunk(s - LAG)
        return carry
    lax.fori_loop(0, N_CHUNK + LAG, step, 0)
    finish_pair(N_CHUNK - 1)

    def result(j):
        t = 3 * chip + j
        zx_copy(j).wait_recv()

        def step(i, c):
            rows = sub_rows(t * HALF, i)
            proj = (own[rows, :].astype(F32) + z_in[sub_rows(j * HALF, i), :].astype(F32)).astype(BF16).astype(F32)
            final = res[rows, :].astype(F32) + rms(proj, gain4).astype(BF16).astype(F32)
            stage[sub_rows(j * HALF, i), :] = final.astype(BF16)
            return c
        lax.fori_loop(0, HALF // SUB, step, 0)

    def keep_copy(j, place):
        return pltpu.make_async_copy(stage.at[pl.ds(j * HALF, HALF)], out_ref.at[pl.ds(place * HALF, HALF)], keep_sem.at[place // 2])

    def give_copy(j):
        return remote(stage.at[pl.ds(j * HALF, HALF)], out_ref.at[pl.ds(HALF, HALF)], out_ss, out_rs, mate)

    for j in range(3):
        result(j)

        @pl.when(core == 0)
        def _():
            (give_copy(j) if j == 2 else keep_copy(j, 2 * j)).start()

        @pl.when(core == 1)
        def _():
            (give_copy(j) if j == 0 else keep_copy(j, 2 * j - 2)).start()

    give_copy(0).wait()
    keep_copy(0, 0).wait()
    keep_copy(0, 2).wait()
    zp_copy(N_CHUNK - 1).wait_send()
    for t in range(N_CHUNK):
        yx_copy(t).wait_send()
    for j in range(3):
        zx_copy(3 * (1 - chip) + j).wait_send()


def run_layer(block_rows, looked, tokens, k_pos, inv_freq, w_query, w_key, w_value, w_out, w_gate, w_up, w_down, g1, g2, g3, g4):
    seq, dim = looked.shape
    scale = float(np.sqrt(np.float32(dim)).astype(jnp.bfloat16))
    vmem = pl.BlockSpec(memory_space=pltpu.VMEM)
    hbm = pl.BlockSpec(memory_space=pl.ANY)
    half_all = pltpu.VMEM((seq // 2, dim), BF16)
    dma = pltpu.SemaphoreType.DMA
    return pl.pallas_call(
        functools.partial(layer_kernel, block_rows, scale),
        name="layer",
        out_shape=jax.ShapeDtypeStruct((seq // 4, dim), BF16),
        in_specs=[hbm] + [vmem] * 3 + [hbm] * 7 + [vmem] * 4,
        out_specs=hbm,
        scratch_shapes=[
            pltpu.VMEM((dim, 1024), BF16),
            pltpu.VMEM(w_out.shape, BF16), pltpu.VMEM(w_gate.shape, BF16), pltpu.VMEM(w_up.shape, BF16),
            pltpu.VMEM(w_down.shape, BF16),
            pltpu.VMEM((2, WQ_ROWS, 2, 256), BF16),
            half_all, half_all, half_all, half_all,
            pltpu.VMEM((4, ROWS, dim), BF16),
            pltpu.VMEM((seq, 256), BF16), pltpu.VMEM((seq, 256), BF16),
            pltpu.VMEM((ROWS, 512), BF16), pltpu.VMEM((ROWS, dim), BF16),
            pltpu.VMEM((HALF, dim), BF16), pltpu.VMEM((HALF, dim), BF16),
            pltpu.VMEM((HALF, dim), BF16), pltpu.VMEM((2, HALF, dim), BF16),
            pltpu.VMEM((3 * HALF, dim), BF16), pltpu.VMEM((3 * HALF, dim), BF16),
            dma((2,)), dma((6,)), dma((N_CHUNK,)), dma((N_CHUNK,)), dma((N_CHUNK,)), dma((N_CHUNK,)), dma((N_CHUNK,)),
            dma((2,)), dma((2,)), dma, dma,
            dma((N_CHUNK,)), dma((N_CHUNK,)), dma((2,)), dma((2,)), dma, dma((2,)),
            dma((3,)), dma((3,)), dma, dma, dma((2,)),
        ],
        compiler_params=pltpu.CompilerParams(
            collective_id=0, has_side_effects=True, vmem_limit_bytes=67043328),
    )(looked, tokens, k_pos, inv_freq, w_query, w_key, w_value, w_out, w_gate, w_up, w_down, g1, g2, g3, g4)


def solution(mesh):
    in_specs = (P("dp", None), P("dp", None), P("tp", None), P(None, "tp", None), P(None, "tp", None), P(None, "tp", None), P("tp", None, None), P(None, "tp"), P(None, "tp"), P("tp", None), P(None), P(None), P(None), P(None))

    def device_step(tokens, positions, embed_block, w_query, w_key, w_value, w_out, w_gate, w_up, w_down, g1, g2, g3, g4):
        model_dim = embed_block.shape[1]
        block_rows = embed_block.shape[0]
        looked = embed_block.at[lax.rem(tokens[0], block_rows)].get(mode='promise_in_bounds')
        inv_freq = (ROPE_BASE ** (-2.0 * np.arange(128) / 256)).astype(np.float32).reshape(1, 128)
        out = run_layer(
            block_rows, looked, tokens, positions, jnp.asarray(inv_freq),
            w_query, w_key.reshape(model_dim, 256), w_value.reshape(model_dim, 256),
            w_out.reshape(512, model_dim), w_gate, w_up, w_down, g1, g2, g3, g4)
        return out[None]

    return jax.shard_map(device_step, mesh=mesh, in_specs=in_specs, out_specs=P("dp", "tp", None), check_vma=False)
```

```python
import functools

import jax
import jax.numpy as jnp
import numpy as np
from jax import lax
from jax.experimental import pallas as pl
from jax.experimental.pallas import tpu as pltpu
from jax.sharding import PartitionSpec as P

WINDOW = 4096
QUERY_SCALE = 256.0 ** -0.5
SOFT_CAP = 50.0
NORM_EPS = 1e-6
ROPE_BASE = 10000.0

N_CHUNK = 6
ROWS = 128
HALF = 64
SUB = 16
PIECES = 4
N_TILE = 512
WQ_ROWS = 256
EARLY = 2
LEAD = 3
LAG = 2
LATE = 4
MESH = pl.DeviceIdType.MESH
F32 = jnp.float32
BF16 = jnp.bfloat16


def rms(block, gain):
    mean_sq = jnp.mean(block * block, axis=-1, keepdims=True)
    return block * lax.rsqrt(mean_sq + NORM_EPS) * gain


def layer_kernel(
    block_rows, scale,
    rows_ref, ids_ref, kpos_ref, freq_ref,
    wq_hbm, wk_hbm, wv_hbm, wo_hbm, wg_hbm, wu_hbm, wd_hbm,
    g1_ref, g2_ref, g3_ref, g4_ref,
    out_ref,
    wqkv, wo, wg, wu, wd,
    wq_in, own, sib, res, y_in, norm, k_all, v_all, o_buf, h_buf, y_out, y_pair, pair_out, pair_in, z_in, stage,
    wq_sem, w_sem, own_sem, sib_ss, sib_rs, ex_ss, ex_rs, a_ss, a_rs, yp_ss, yp_rs,
    yx_ss, yx_rs, m_ss, m_rs, zp_ss, zp_rs, zx_ss, zx_rs, out_ss, out_rs, keep_sem,
    stage_sem, first_ss, first_rs, ex0_ss, ex0_rs,
):
    dp = lax.axis_index("dp")
    tp = lax.axis_index("tp")
    chip = lax.div(tp, 2)
    core = lax.rem(tp, 2)
    mate = 2 * chip + 1 - core
    far = 2 * (1 - chip) + core

    def remote(src, dst, send_sem, recv_sem, target):
        return pltpu.make_async_remote_copy(
            src_ref=src, dst_ref=dst, send_sem=send_sem, recv_sem=recv_sem,
            device_id=(dp, target), device_id_type=MESH)

    def half_rows(t):
        return pl.ds(pl.multiple_of(t * HALF, HALF), HALF)

    mine = pl.ds(pl.multiple_of(core * HALF, HALF), HALF)

    def own_copy(t):
        rows = pl.ds(pl.multiple_of(t * ROWS + core * HALF, HALF), HALF)
        return pltpu.make_async_copy(rows_ref.at[rows], own.at[half_rows(t)], own_sem.at[t])

    def sib_copy(t):
        rows = pl.ds(pl.multiple_of(t * ROWS + (1 - core) * HALF, HALF), HALF)
        return remote(rows_ref.at[rows], sib.at[half_rows(t)], sib_ss.at[t], sib_rs.at[t], mate)

    def piece_rows(i, base=0):
        return pl.ds(pl.multiple_of(base + i * SUB, SUB), SUB)

    def stage_copy(i):
        rows = pl.ds(pl.multiple_of((1 - core) * HALF + i * SUB, SUB), SUB)
        return pltpu.make_async_copy(rows_ref.at[rows], y_out.at[piece_rows(i)], stage_sem.at[i])

    def sib_first(i):
        return remote(y_out.at[piece_rows(i)], sib.at[piece_rows(i)], first_ss.at[i], first_rs.at[i], mate)

    def ex_first(i):
        return remote(own.at[piece_rows(i)], res.at[piece_rows(i)], ex0_ss.at[i], ex0_rs.at[i], far)

    def ex_copy(t):
        return remote(own.at[half_rows(t)], res.at[half_rows(t)], ex_ss.at[t], ex_rs.at[t], far)

    def norm_copy(slot, send_sem, recv_sem):
        return remote(norm.at[slot, mine], norm.at[slot, mine], send_sem, recv_sem, mate)

    def yp_copy():
        return remote(y_out, y_pair, yp_ss, yp_rs, mate)

    def yx_copy(t):
        return remote(sib.at[half_rows(t)], y_in.at[half_rows(t)], yx_ss.at[t], yx_rs.at[t], far)

    def m_copy(t):
        slot = lax.rem(t, 2)
        return norm_copy(slot, m_ss.at[slot], m_rs.at[slot])

    def zp_copy(t):
        slot = lax.rem(t, 2)
        return remote(pair_out, pair_in.at[slot], zp_ss, zp_rs.at[slot], mate)

    def zx_copy(t, i):
        j = lax.rem(t, 3)
        return remote(own.at[piece_rows(i, t * HALF)], z_in.at[piece_rows(i, j * HALF)], zx_ss.at[j, i], zx_rs.at[j, i], far)

    weights = [
        pltpu.make_async_copy(src, dst, w_sem.at[i])
        for i, (src, dst) in enumerate(
            [(wk_hbm, wqkv.at[:, pl.ds(512, 256)]), (wv_hbm, wqkv.at[:, pl.ds(768, 256)]), (wo_hbm, wo), (wg_hbm, wg), (wu_hbm, wu), (wd_hbm, wd)])
    ]

    for i in range(PIECES):
        stage_copy(i).start()
    own_copy(0).start()
    barrier = pltpu.get_barrier_semaphore()
    for peer in (mate, far):
        pl.semaphore_signal(barrier, inc=1, device_id=(dp, peer), device_id_type=MESH)
    pl.semaphore_wait(barrier, 2)

    for i in range(PIECES):
        stage_copy(i).wait()
        sib_first(i).start()
    for t in range(1, N_CHUNK):
        sib_copy(t).start()
        own_copy(t).start()

    def wq_copy(i):
        slot = lax.rem(i, 2)
        rows = pl.ds(pl.multiple_of(i * WQ_ROWS, WQ_ROWS), WQ_ROWS)
        return pltpu.make_async_copy(wq_hbm.at[rows], wq_in.at[slot], wq_sem.at[slot])

    wq_copy(0).start()
    wq_copy(1).start()
    for copy in weights[:3]:
        copy.start()

    def sub_rows(base, i):
        return pl.ds(pl.multiple_of(base + i * SUB, SUB), SUB)

    def combine(dst, other, dst_base, other_base):
        def step(i, carry):
            rows = sub_rows(dst_base, i)
            total = dst[rows, :].astype(F32) + other[sub_rows(other_base, i), :].astype(F32)
            dst[rows, :] = total.astype(BF16)
            return carry
        lax.fori_loop(0, HALF // SUB, step, 0)

    def column(row_ref, t):
        rows = pl.ds(pl.multiple_of(t * ROWS, ROWS), ROWS)
        return jnp.broadcast_to(row_ref[:, rows], (8, ROWS)).T[:, :1]

    def owners(t):
        ids = column(ids_ref, t)
        ids = jnp.where(core == 0, ids[:HALF], ids[HALF:])
        local, local_mate = ids - tp * block_rows, ids - mate * block_rows
        held = (local >= 0) & (local < block_rows)
        held_mate = (local_mate >= 0) & (local_mate < block_rows)
        return held, held_mate

    def pick_rows(rows, held, held_mate):
        looked = jnp.where(held, own[rows, :].astype(F32), jnp.where(held_mate, sib[rows, :].astype(F32), 0.0))
        own[rows, :] = (looked * scale).astype(BF16)

    held, held_mate = owners(0)
    own_copy(0).wait()
    for i in range(PIECES):
        part = slice(i * SUB, (i + 1) * SUB)
        sib_first(i).wait_recv()
        pick_rows(pl.ds(i * SUB, SUB), held[part], held_mate[part])
        ex_first(i).start()

    def send_embed(t, carry):
        held, held_mate = owners(t)
        own_copy(t).wait()
        sib_copy(t).wait_recv()
        for r in range(0, HALF, SUB):
            part = slice(r, r + SUB)
            pick_rows(pl.ds(pl.multiple_of(t * HALF + r, SUB), SUB), held[part], held_mate[part])

        @pl.when(t < LEAD)
        def _():
            ex_copy(t).start()
        return carry
    lax.fori_loop(1, N_CHUNK, send_embed, 0)

    k_all[...] = jnp.zeros_like(k_all)
    v_all[...] = jnp.zeros_like(v_all)
    gain1, gain2, gain3, gain4 = [(1.0 + g[...]).reshape(1, -1) for g in (g1_ref, g2_ref, g3_ref, g4_ref)]

    out_row = lax.broadcasted_iota(jnp.int32, (256, 256), 0)
    in_row = lax.broadcasted_iota(jnp.int32, (256, 256), 1)
    split_heads = jnp.where(in_row == jnp.where(out_row < 128, 2 * out_row, 2 * out_row - 255), 1.0, 0.0).astype(BF16)

    def spread_wq(i, carry):
        slot = lax.rem(i, 2)
        wq_copy(i).wait()
        for r in range(0, WQ_ROWS, 128):
            rows = pl.ds(pl.multiple_of(i * WQ_ROWS + r, 128), 128)
            both = wq_in[slot, r:r + 128].reshape(256, 256)
            both = jnp.dot(split_heads, both, preferred_element_type=F32).astype(BF16)
            wqkv[rows, :256] = both[:128]
            wqkv[rows, 256:512] = both[128:]

        @pl.when(i + 2 < 2560 // WQ_ROWS)
        def _():
            wq_copy(i + 2).start()
        return carry
    lax.fori_loop(0, 2560 // WQ_ROWS, spread_wq, 0)
    for copy in weights[3:]:
        copy.start()
    for i in range(PIECES):
        sib_first(i).wait_send()
    for t in range(1, N_CHUNK):
        sib_copy(t).wait_send()
    for copy in weights[:3]:
        copy.wait()

    def rope(states, cos_tab, sin_tab):
        lower, upper = states[:, :128], states[:, 128:]
        return lower * cos_tab - upper * sin_tab, upper * cos_tab + lower * sin_tab

    def split_halves(both):
        top, bottom = both[:HALF], both[HALF:]
        return jnp.where(core == 0, top, bottom), jnp.where(core == 0, bottom, top)

    def a_copy(t):
        slot = lax.rem(t, 2)
        return norm_copy(2 + slot, a_ss.at[slot], a_rs.at[slot])

    def embed_in(t):
        base = t * HALF
        slot = 2 + lax.rem(t, 2)

        @pl.when(t == 0)
        def _():
            for i in range(PIECES):
                ex_first(i).wait_recv()

        @pl.when(t > 0)
        def _():
            ex_copy(t).wait_recv()

        def embed_step(i, c):
            rows = sub_rows(base, i)
            embed = own[rows, :].astype(F32) + res[rows, :].astype(F32)
            res[rows, :] = embed.astype(BF16)
            norm[slot, sub_rows(core * HALF, i), :] = rms(embed, gain1).astype(BF16)
            return c
        lax.fori_loop(0, HALF // SUB, embed_step, 0)
        a_copy(t).start()

    def attention_chunk(t):
        slot = 2 + lax.rem(t, 2)
        rows = pl.ds(pl.multiple_of(t * ROWS, ROWS), ROWS)

        @pl.when(t <= LAG)
        def _():
            embed_in(t)
        q_pos = column(kpos_ref, t)
        angles = q_pos.astype(F32) * freq_ref[...]
        cos_tab, sin_tab = jnp.cos(angles), jnp.sin(angles)
        offset = q_pos - kpos_ref[...]
        keep = (offset >= 0) & (offset < WINDOW)
        a_copy(t).wait()
        proj = jnp.dot(norm[slot], wqkv[:, 512:], preferred_element_type=F32)
        lower, upper = rope(proj[:, :256], cos_tab, sin_tab)
        k_all[rows, :128] = lower.astype(BF16)
        k_all[rows, 128:] = upper.astype(BF16)
        v_all[rows, :] = proj[:, 256:].astype(BF16)
        proj = jnp.dot(norm[slot], wqkv[:, :512], preferred_element_type=F32)
        for head in range(2):
            lower, upper = rope(proj[:, head * 256:(head + 1) * 256], cos_tab, sin_tab)
            query = jnp.concatenate([(lower * QUERY_SCALE).astype(BF16), (upper * QUERY_SCALE).astype(BF16)], axis=-1)
            scores = lax.dot_general(query, k_all[...], (((1,), (1,)), ((), ())), preferred_element_type=F32)
            weight = jnp.where(keep, jnp.exp(SOFT_CAP * jnp.tanh(scores * (1.0 / SOFT_CAP))), 0.0)
            weight = weight * (1.0 / jnp.sum(weight, axis=-1, keepdims=True))
            mixed = jnp.dot(weight.astype(BF16), v_all[...], preferred_element_type=F32)
            o_buf[:, head * 256:(head + 1) * 256] = mixed.astype(BF16)

        def out_tile(n, c):
            cols = pl.ds(pl.multiple_of(n * N_TILE, N_TILE), N_TILE)
            both = jnp.dot(o_buf[...], wo[:, cols], preferred_element_type=F32).astype(BF16)
            sib[half_rows(t), cols], y_out[:, cols] = split_halves(both)
            return c
        lax.fori_loop(0, 2560 // N_TILE, out_tile, 0, unroll=True)
        yp_copy().start()

    def send_proj(t):
        yp_copy().wait()
        combine(sib, y_pair, t * HALF, 0)
        yx_copy(t).start()

        @pl.when(t + LEAD < N_CHUNK)
        def _():
            ex_copy(t + LEAD).start()

    def mlp_in(t):
        base = t * HALF
        slot = lax.rem(t, 2)
        yx_copy(t).wait_recv()

        def step(i, c):
            rows = sub_rows(base, i)
            proj = (sib[rows, :].astype(F32) + y_in[rows, :].astype(F32)).astype(BF16).astype(F32)
            resid = (res[rows, :].astype(F32) + rms(proj, gain2).astype(BF16).astype(F32)).astype(BF16)
            res[rows, :] = resid
            norm[slot, sub_rows(core * HALF, i), :] = rms(resid.astype(F32), gain3).astype(BF16)
            return c
        lax.fori_loop(0, HALF // SUB, step, 0)
        m_copy(t).start()

    def finish_pair(t):
        zp_copy(t).wait_recv()
        combine(own, pair_in.at[lax.rem(t, 2)], t * HALF, 0)

        @pl.when((lax.div(t, 3) != chip) & (t >= LAG))
        def _():
            for i in range(PIECES):
                zx_copy(t, i).start()

    def mlp_chunk(t):
        slot = lax.rem(t, 2)

        @pl.when(t == 0)
        def _():
            for copy in weights[3:]:
                copy.wait()
            for i in range(PIECES):
                ex_first(i).wait_send()

        @pl.when(t > 0)
        def _():
            ex_copy(t).wait_send()
        m_copy(t).wait()

        def gate_tile(n, c):
            cols = pl.ds(pl.multiple_of(n * N_TILE, N_TILE), N_TILE)
            gate = jnp.dot(norm[slot], wg[:, cols], preferred_element_type=F32)
            up = jnp.dot(norm[slot], wu[:, cols], preferred_element_type=F32)
            h_buf[:, cols] = (jax.nn.gelu(gate, approximate=True) * up).astype(BF16)
            return c
        lax.fori_loop(0, EARLY, gate_tile, 0, unroll=True)

        @pl.when(t > 0)
        def _():
            finish_pair(t - 1)
        lax.fori_loop(EARLY, 2560 // N_TILE, gate_tile, 0, unroll=True)

        @pl.when(t + LAG + 1 < N_CHUNK)
        def _():
            embed_in(t + LAG + 1)

        @pl.when((t + 1 >= LATE) & (t < N_CHUNK - 1))
        def _():
            mlp_in(t + 1)

        @pl.when(t > 0)
        def _():
            zp_copy(t - 1).wait_send()

        def down_tile(n, c):
            cols = pl.ds(pl.multiple_of(n * N_TILE, N_TILE), N_TILE)
            both = jnp.dot(h_buf[...], wd[:, cols], preferred_element_type=F32).astype(BF16)
            own[half_rows(t), cols], pair_out[:, cols] = split_halves(both)
            return c
        lax.fori_loop(0, 2560 // N_TILE, down_tile, 0, unroll=True)
        zp_copy(t).start()

    def step(s, carry):
        @pl.when(s < N_CHUNK)
        def _():
            attention_chunk(s)

        @pl.when((s >= LAG) & (s < LATE + LAG))
        def _():
            mlp_in(s - LAG)

        @pl.when(s < N_CHUNK)
        def _():
            send_proj(s)

        @pl.when((s == N_CHUNK - 1) & (chip != 0))
        def _():
            for t in range(LAG):
                for i in range(PIECES):
                    zx_copy(t, i).start()

        @pl.when(s >= LAG)
        def _():
            mlp_chunk(s - LAG)
        return carry
    lax.fori_loop(0, N_CHUNK + LAG, step, 0)
    finish_pair(N_CHUNK - 1)

    def keep_copy(j, place, i):
        rows = piece_rows(i, j * HALF)
        return pltpu.make_async_copy(stage.at[rows], out_ref.at[piece_rows(i, place * HALF)], keep_sem.at[place // 2, i])

    def give_copy(j, i):
        return remote(stage.at[piece_rows(i, j * HALF)], out_ref.at[piece_rows(i, HALF)], out_ss.at[i], out_rs.at[i], mate)

    for j in range(3):
        def step(i, c):
            zx_copy(j, i).wait_recv()
            rows = sub_rows((3 * chip + j) * HALF, i)
            proj = (own[rows, :].astype(F32) + z_in[sub_rows(j * HALF, i), :].astype(F32)).astype(BF16).astype(F32)
            final = res[rows, :].astype(F32) + rms(proj, gain4).astype(BF16).astype(F32)
            stage[sub_rows(j * HALF, i), :] = final.astype(BF16)

            @pl.when(core == 0)
            def _():
                (give_copy(j, i) if j == 2 else keep_copy(j, 2 * j, i)).start()

            @pl.when(core == 1)
            def _():
                (give_copy(j, i) if j == 0 else keep_copy(j, 2 * j - 2, i)).start()
            return c
        lax.fori_loop(0, PIECES, step, 0)

    for i in range(PIECES):
        give_copy(0, i).wait()
        keep_copy(0, 0, i).wait()
        keep_copy(0, 2, i).wait()
    zp_copy(N_CHUNK - 1).wait_send()
    for t in range(N_CHUNK):
        yx_copy(t).wait_send()
    for j in range(3):
        for i in range(PIECES):
            zx_copy(3 * (1 - chip) + j, i).wait_send()


def run_layer(block_rows, looked, tokens, k_pos, inv_freq, w_query, w_key, w_value, w_out, w_gate, w_up, w_down, g1, g2, g3, g4):
    seq, dim = looked.shape
    scale = float(np.sqrt(np.float32(dim)).astype(jnp.bfloat16))
    vmem = pl.BlockSpec(memory_space=pltpu.VMEM)
    hbm = pl.BlockSpec(memory_space=pl.ANY)
    half_all = pltpu.VMEM((seq // 2, dim), BF16)
    dma = pltpu.SemaphoreType.DMA
    return pl.pallas_call(
        functools.partial(layer_kernel, block_rows, scale),
        name="layer",
        out_shape=jax.ShapeDtypeStruct((seq // 4, dim), BF16),
        in_specs=[hbm] + [vmem] * 3 + [hbm] * 7 + [vmem] * 4,
        out_specs=hbm,
        scratch_shapes=[
            pltpu.VMEM((dim, 1024), BF16),
            pltpu.VMEM(w_out.shape, BF16), pltpu.VMEM(w_gate.shape, BF16), pltpu.VMEM(w_up.shape, BF16),
            pltpu.VMEM(w_down.shape, BF16),
            pltpu.VMEM((2, WQ_ROWS, 2, 256), BF16),
            half_all, half_all, half_all, half_all,
            pltpu.VMEM((4, ROWS, dim), BF16),
            pltpu.VMEM((seq, 256), BF16), pltpu.VMEM((seq, 256), BF16),
            pltpu.VMEM((ROWS, 512), BF16), pltpu.VMEM((ROWS, dim), BF16),
            pltpu.VMEM((HALF, dim), BF16), pltpu.VMEM((HALF, dim), BF16),
            pltpu.VMEM((HALF, dim), BF16), pltpu.VMEM((2, HALF, dim), BF16),
            pltpu.VMEM((3 * HALF, dim), BF16), pltpu.VMEM((3 * HALF, dim), BF16),
            dma((2,)), dma((6,)), dma((N_CHUNK,)), dma((N_CHUNK,)), dma((N_CHUNK,)), dma((N_CHUNK,)), dma((N_CHUNK,)),
            dma((2,)), dma((2,)), dma, dma,
            dma((N_CHUNK,)), dma((N_CHUNK,)), dma((2,)), dma((2,)), dma, dma((2,)),
            dma((3, PIECES)), dma((3, PIECES)), dma((PIECES,)), dma((PIECES,)), dma((2, PIECES)),
            dma((PIECES,)), dma((PIECES,)), dma((PIECES,)), dma((PIECES,)), dma((PIECES,)),
        ],
        compiler_params=pltpu.CompilerParams(
            collective_id=0, has_side_effects=True, vmem_limit_bytes=67043328),
    )(looked, tokens, k_pos, inv_freq, w_query, w_key, w_value, w_out, w_gate, w_up, w_down, g1, g2, g3, g4)


def solution(mesh):
    in_specs = (P("dp", None), P("dp", None), P("tp", None), P(None, "tp", None), P(None, "tp", None), P(None, "tp", None), P("tp", None, None), P(None, "tp"), P(None, "tp"), P("tp", None), P(None), P(None), P(None), P(None))

    def device_step(tokens, positions, embed_block, w_query, w_key, w_value, w_out, w_gate, w_up, w_down, g1, g2, g3, g4):
        model_dim = embed_block.shape[1]
        block_rows = embed_block.shape[0]
        looked = embed_block.at[lax.rem(tokens[0], block_rows)].get(mode='promise_in_bounds')
        inv_freq = (ROPE_BASE ** (-2.0 * np.arange(128) / 256)).astype(np.float32).reshape(1, 128)
        out = run_layer(
            block_rows, looked, tokens, positions, jnp.asarray(inv_freq),
            w_query, w_key.reshape(model_dim, 256), w_value.reshape(model_dim, 256),
            w_out.reshape(512, model_dim), w_gate, w_up, w_down, g1, g2, g3, g4)
        return out[None]

    return jax.shard_map(device_step, mesh=mesh, in_specs=in_specs, out_specs=P("dp", "tp", None), check_vma=False)
```

```python
import functools

import jax
import jax.numpy as jnp
import numpy as np
from jax import lax
from jax.experimental import pallas as pl
from jax.experimental.pallas import tpu as pltpu
from jax.sharding import PartitionSpec as P

WINDOW = 4096
QUERY_SCALE = 256.0 ** -0.5
SOFT_CAP = 50.0
NORM_EPS = 1e-6
ROPE_BASE = 10000.0

N_CHUNK = 6
ROWS = 128
HALF = 64
SUB = 16
PIECES = 4
N_TILE = 512
WQ_ROWS = 256
EARLY = 2
LEAD = 3
LAG = 2
LATE = 4
MESH = pl.DeviceIdType.MESH
F32 = jnp.float32
BF16 = jnp.bfloat16


def rms(block, gain):
    mean_sq = jnp.mean(block * block, axis=-1, keepdims=True)
    return block * lax.rsqrt(mean_sq + NORM_EPS) * gain


def layer_kernel(
    block_rows, scale,
    rows_ref, ids_hbm, kpos_hbm, freq_hbm,
    wq_hbm, wk_hbm, wv_hbm, wo_hbm, wg_hbm, wu_hbm, wd_hbm,
    g1_hbm, g2_hbm, g3_hbm, g4_hbm,
    out_ref,
    ids_ref, kpos_ref, freq_ref, g1_ref, g2_ref, g3_ref, g4_ref,
    wqkv, wo, wg, wu, wd,
    wq_in, own, sib, res, y_in, norm, k_all, v_all, o_buf, h_buf, y_out, y_pair, pair_out, pair_in, z_in, stage,
    wq_sem, w_sem, own_sem, sib_ss, sib_rs, ex_ss, ex_rs, a_ss, a_rs, yp_ss, yp_rs,
    yx_ss, yx_rs, m_ss, m_rs, zp_ss, zp_rs, zx_ss, zx_rs, out_ss, out_rs, keep_sem,
    small_sem, stage_sem, first_ss, first_rs, ex0_ss, ex0_rs,
):
    dp = lax.axis_index("dp")
    tp = lax.axis_index("tp")
    chip = lax.div(tp, 2)
    core = lax.rem(tp, 2)
    mate = 2 * chip + 1 - core
    far = 2 * (1 - chip) + core

    def remote(src, dst, send_sem, recv_sem, target):
        return pltpu.make_async_remote_copy(
            src_ref=src, dst_ref=dst, send_sem=send_sem, recv_sem=recv_sem,
            device_id=(dp, target), device_id_type=MESH)

    def half_rows(t):
        return pl.ds(pl.multiple_of(t * HALF, HALF), HALF)

    mine = pl.ds(pl.multiple_of(core * HALF, HALF), HALF)

    def own_copy(t):
        rows = pl.ds(pl.multiple_of(t * ROWS + core * HALF, HALF), HALF)
        return pltpu.make_async_copy(rows_ref.at[rows], own.at[half_rows(t)], own_sem.at[t])

    def sib_copy(t):
        rows = pl.ds(pl.multiple_of(t * ROWS + (1 - core) * HALF, HALF), HALF)
        return remote(rows_ref.at[rows], sib.at[half_rows(t)], sib_ss.at[t], sib_rs.at[t], mate)

    def piece_rows(i, base=0):
        return pl.ds(pl.multiple_of(base + i * SUB, SUB), SUB)

    def stage_copy(i):
        rows = pl.ds(pl.multiple_of((1 - core) * HALF + i * SUB, SUB), SUB)
        return pltpu.make_async_copy(rows_ref.at[rows], y_out.at[piece_rows(i)], stage_sem.at[i])

    def sib_first(i):
        return remote(y_out.at[piece_rows(i)], sib.at[piece_rows(i)], first_ss.at[i], first_rs.at[i], mate)

    def ex_first(i):
        return remote(own.at[piece_rows(i)], res.at[piece_rows(i)], ex0_ss.at[i], ex0_rs.at[i], far)

    def ex_copy(t):
        return remote(own.at[half_rows(t)], res.at[half_rows(t)], ex_ss.at[t], ex_rs.at[t], far)

    def norm_copy(slot, send_sem, recv_sem):
        return remote(norm.at[slot, mine], norm.at[slot, mine], send_sem, recv_sem, mate)

    def yp_copy():
        return remote(y_out, y_pair, yp_ss, yp_rs, mate)

    def yx_copy(t):
        return remote(sib.at[half_rows(t)], y_in.at[half_rows(t)], yx_ss.at[t], yx_rs.at[t], far)

    def m_copy(t):
        slot = lax.rem(t, 2)
        return norm_copy(slot, m_ss.at[slot], m_rs.at[slot])

    def zp_copy(t):
        slot = lax.rem(t, 2)
        return remote(pair_out, pair_in.at[slot], zp_ss, zp_rs.at[slot], mate)

    def zx_copy(t, i):
        j = lax.rem(t, 3)
        return remote(own.at[piece_rows(i, t * HALF)], z_in.at[piece_rows(i, j * HALF)], zx_ss.at[j, i], zx_rs.at[j, i], far)

    weights = [
        pltpu.make_async_copy(src, dst, w_sem.at[i])
        for i, (src, dst) in enumerate(
            [(wk_hbm, wqkv.at[:, pl.ds(512, 256)]), (wv_hbm, wqkv.at[:, pl.ds(768, 256)]), (wo_hbm, wo), (wg_hbm, wg), (wu_hbm, wu), (wd_hbm, wd)])
    ]

    for i in range(PIECES):
        stage_copy(i).start()
    own_copy(0).start()
    small = [
        pltpu.make_async_copy(src, dst, small_sem.at[i])
        for i, (src, dst) in enumerate([
            (ids_hbm, ids_ref), (kpos_hbm, kpos_ref), (freq_hbm, freq_ref),
            (g1_hbm, g1_ref), (g2_hbm, g2_ref), (g3_hbm, g3_ref), (g4_hbm, g4_ref)])
    ]
    for copy in small:
        copy.start()
    barrier = pltpu.get_barrier_semaphore()
    for peer in (mate, far):
        pl.semaphore_signal(barrier, inc=1, device_id=(dp, peer), device_id_type=MESH)
    pl.semaphore_wait(barrier, 2)

    for i in range(PIECES):
        stage_copy(i).wait()
        sib_first(i).start()
    for t in range(1, N_CHUNK):
        sib_copy(t).start()
        own_copy(t).start()

    def wq_copy(i):
        slot = lax.rem(i, 2)
        rows = pl.ds(pl.multiple_of(i * WQ_ROWS, WQ_ROWS), WQ_ROWS)
        return pltpu.make_async_copy(wq_hbm.at[rows], wq_in.at[slot], wq_sem.at[slot])

    wq_copy(0).start()
    wq_copy(1).start()
    for copy in weights[:3]:
        copy.start()

    def sub_rows(base, i):
        return pl.ds(pl.multiple_of(base + i * SUB, SUB), SUB)

    def combine(dst, other, dst_base, other_base):
        def step(i, carry):
            rows = sub_rows(dst_base, i)
            total = dst[rows, :].astype(F32) + other[sub_rows(other_base, i), :].astype(F32)
            dst[rows, :] = total.astype(BF16)
            return carry
        lax.fori_loop(0, HALF // SUB, step, 0)

    def column(row_ref, t):
        rows = pl.ds(pl.multiple_of(t * ROWS, ROWS), ROWS)
        return jnp.broadcast_to(row_ref[:, rows], (8, ROWS)).T[:, :1]

    def owners(t):
        ids = column(ids_ref, t)
        ids = jnp.where(core == 0, ids[:HALF], ids[HALF:])
        local, local_mate = ids - tp * block_rows, ids - mate * block_rows
        held = (local >= 0) & (local < block_rows)
        held_mate = (local_mate >= 0) & (local_mate < block_rows)
        return held, held_mate

    def pick_rows(rows, held, held_mate):
        looked = jnp.where(held, own[rows, :].astype(F32), jnp.where(held_mate, sib[rows, :].astype(F32), 0.0))
        own[rows, :] = (looked * scale).astype(BF16)

    small[0].wait()
    held, held_mate = owners(0)
    own_copy(0).wait()
    for i in range(PIECES):
        part = slice(i * SUB, (i + 1) * SUB)
        sib_first(i).wait_recv()
        pick_rows(pl.ds(i * SUB, SUB), held[part], held_mate[part])
        ex_first(i).start()

    def send_embed(t, carry):
        held, held_mate = owners(t)
        own_copy(t).wait()
        sib_copy(t).wait_recv()
        for r in range(0, HALF, SUB):
            part = slice(r, r + SUB)
            pick_rows(pl.ds(pl.multiple_of(t * HALF + r, SUB), SUB), held[part], held_mate[part])

        @pl.when(t < LEAD)
        def _():
            ex_copy(t).start()
        return carry
    lax.fori_loop(1, N_CHUNK, send_embed, 0)

    for copy in small[1:]:
        copy.wait()
    k_all[...] = jnp.zeros_like(k_all)
    v_all[...] = jnp.zeros_like(v_all)
    gain1, gain2, gain3, gain4 = [(1.0 + g[...]).reshape(1, -1) for g in (g1_ref, g2_ref, g3_ref, g4_ref)]

    out_row = lax.broadcasted_iota(jnp.int32, (256, 256), 0)
    in_row = lax.broadcasted_iota(jnp.int32, (256, 256), 1)
    split_heads = jnp.where(in_row == jnp.where(out_row < 128, 2 * out_row, 2 * out_row - 255), 1.0, 0.0).astype(BF16)

    def spread_wq(i, carry):
        slot = lax.rem(i, 2)
        wq_copy(i).wait()
        for r in range(0, WQ_ROWS, 128):
            rows = pl.ds(pl.multiple_of(i * WQ_ROWS + r, 128), 128)
            both = wq_in[slot, r:r + 128].reshape(256, 256)
            both = jnp.dot(split_heads, both, preferred_element_type=F32).astype(BF16)
            wqkv[rows, :256] = both[:128]
            wqkv[rows, 256:512] = both[128:]

        @pl.when(i + 2 < 2560 // WQ_ROWS)
        def _():
            wq_copy(i + 2).start()
        return carry
    lax.fori_loop(0, 2560 // WQ_ROWS, spread_wq, 0)
    for copy in weights[3:]:
        copy.start()
    for i in range(PIECES):
        sib_first(i).wait_send()
    for t in range(1, N_CHUNK):
        sib_copy(t).wait_send()
    for copy in weights[:3]:
        copy.wait()

    def rope(states, cos_tab, sin_tab):
        lower, upper = states[:, :128], states[:, 128:]
        return lower * cos_tab - upper * sin_tab, upper * cos_tab + lower * sin_tab

    def split_halves(both):
        top, bottom = both[:HALF], both[HALF:]
        return jnp.where(core == 0, top, bottom), jnp.where(core == 0, bottom, top)

    def a_copy(t):
        slot = lax.rem(t, 2)
        return norm_copy(2 + slot, a_ss.at[slot], a_rs.at[slot])

    def embed_in(t):
        base = t * HALF
        slot = 2 + lax.rem(t, 2)

        @pl.when(t == 0)
        def _():
            for i in range(PIECES):
                ex_first(i).wait_recv()

        @pl.when(t > 0)
        def _():
            ex_copy(t).wait_recv()

        def embed_step(i, c):
            rows = sub_rows(base, i)
            embed = own[rows, :].astype(F32) + res[rows, :].astype(F32)
            res[rows, :] = embed.astype(BF16)
            norm[slot, sub_rows(core * HALF, i), :] = rms(embed, gain1).astype(BF16)
            return c
        lax.fori_loop(0, HALF // SUB, embed_step, 0)
        a_copy(t).start()

    def attention_chunk(t):
        slot = 2 + lax.rem(t, 2)
        rows = pl.ds(pl.multiple_of(t * ROWS, ROWS), ROWS)

        @pl.when(t <= LAG)
        def _():
            embed_in(t)
        q_pos = column(kpos_ref, t)
        angles = q_pos.astype(F32) * freq_ref[...]
        cos_tab, sin_tab = jnp.cos(angles), jnp.sin(angles)
        offset = q_pos - kpos_ref[...]
        keep = (offset >= 0) & (offset < WINDOW)
        a_copy(t).wait()
        proj = jnp.dot(norm[slot], wqkv[:, 512:], preferred_element_type=F32)
        lower, upper = rope(proj[:, :256], cos_tab, sin_tab)
        k_all[rows, :128] = lower.astype(BF16)
        k_all[rows, 128:] = upper.astype(BF16)
        v_all[rows, :] = proj[:, 256:].astype(BF16)
        proj = jnp.dot(norm[slot], wqkv[:, :512], preferred_element_type=F32)
        for head in range(2):
            lower, upper = rope(proj[:, head * 256:(head + 1) * 256], cos_tab, sin_tab)
            query = jnp.concatenate([(lower * QUERY_SCALE).astype(BF16), (upper * QUERY_SCALE).astype(BF16)], axis=-1)
            scores = lax.dot_general(query, k_all[...], (((1,), (1,)), ((), ())), preferred_element_type=F32)
            weight = jnp.where(keep, jnp.exp(SOFT_CAP * jnp.tanh(scores * (1.0 / SOFT_CAP))), 0.0)
            weight = weight * (1.0 / jnp.sum(weight, axis=-1, keepdims=True))
            mixed = jnp.dot(weight.astype(BF16), v_all[...], preferred_element_type=F32)
            o_buf[:, head * 256:(head + 1) * 256] = mixed.astype(BF16)

        def out_tile(n, c):
            cols = pl.ds(pl.multiple_of(n * N_TILE, N_TILE), N_TILE)
            both = jnp.dot(o_buf[...], wo[:, cols], preferred_element_type=F32).astype(BF16)
            sib[half_rows(t), cols], y_out[:, cols] = split_halves(both)
            return c
        lax.fori_loop(0, 2560 // N_TILE, out_tile, 0, unroll=True)
        yp_copy().start()

    def send_proj(t):
        yp_copy().wait()
        combine(sib, y_pair, t * HALF, 0)
        yx_copy(t).start()

        @pl.when(t + LEAD < N_CHUNK)
        def _():
            ex_copy(t + LEAD).start()

    def mlp_in(t):
        base = t * HALF
        slot = lax.rem(t, 2)
        yx_copy(t).wait_recv()

        def step(i, c):
            rows = sub_rows(base, i)
            proj = (sib[rows, :].astype(F32) + y_in[rows, :].astype(F32)).astype(BF16).astype(F32)
            resid = (res[rows, :].astype(F32) + rms(proj, gain2).astype(BF16).astype(F32)).astype(BF16)
            res[rows, :] = resid
            norm[slot, sub_rows(core * HALF, i), :] = rms(resid.astype(F32), gain3).astype(BF16)
            return c
        lax.fori_loop(0, HALF // SUB, step, 0)
        m_copy(t).start()

    def finish_pair(t):
        zp_copy(t).wait_recv()
        combine(own, pair_in.at[lax.rem(t, 2)], t * HALF, 0)

        @pl.when((lax.div(t, 3) != chip) & (t >= LAG))
        def _():
            for i in range(PIECES):
                zx_copy(t, i).start()

        @pl.when((t == LAG) & (chip != 0))
        def _():
            for early in range(LAG):
                for i in range(PIECES):
                    zx_copy(early, i).start()

    def mlp_chunk(t):
        slot = lax.rem(t, 2)

        @pl.when(t == 0)
        def _():
            for copy in weights[3:]:
                copy.wait()
            for i in range(PIECES):
                ex_first(i).wait_send()

        @pl.when(t > 0)
        def _():
            ex_copy(t).wait_send()
        m_copy(t).wait()

        def gate_tile(n, c):
            cols = pl.ds(pl.multiple_of(n * N_TILE, N_TILE), N_TILE)
            gate = jnp.dot(norm[slot], wg[:, cols], preferred_element_type=F32)
            up = jnp.dot(norm[slot], wu[:, cols], preferred_element_type=F32)
            h_buf[:, cols] = (jax.nn.gelu(gate, approximate=True) * up).astype(BF16)
            return c
        lax.fori_loop(0, EARLY, gate_tile, 0, unroll=True)

        @pl.when(t > 0)
        def _():
            finish_pair(t - 1)
        lax.fori_loop(EARLY, 2560 // N_TILE, gate_tile, 0, unroll=True)

        @pl.when(t + LAG + 1 < N_CHUNK)
        def _():
            embed_in(t + LAG + 1)

        @pl.when((t + 1 >= LATE) & (t < N_CHUNK - 1))
        def _():
            mlp_in(t + 1)

        @pl.when(t > 0)
        def _():
            zp_copy(t - 1).wait_send()

        def down_tile(n, c):
            cols = pl.ds(pl.multiple_of(n * N_TILE, N_TILE), N_TILE)
            both = jnp.dot(h_buf[...], wd[:, cols], preferred_element_type=F32).astype(BF16)
            own[half_rows(t), cols], pair_out[:, cols] = split_halves(both)
            return c
        lax.fori_loop(0, 2560 // N_TILE, down_tile, 0, unroll=True)
        zp_copy(t).start()

    def step(s, carry):
        @pl.when(s < N_CHUNK)
        def _():
            attention_chunk(s)

        @pl.when((s >= LAG) & (s < LATE + LAG))
        def _():
            mlp_in(s - LAG)

        @pl.when(s < N_CHUNK)
        def _():
            send_proj(s)

        @pl.when(s >= LAG)
        def _():
            mlp_chunk(s - LAG)
        return carry
    lax.fori_loop(0, N_CHUNK + LAG, step, 0)
    finish_pair(N_CHUNK - 1)

    def keep_copy(j, place, i):
        rows = piece_rows(i, j * HALF)
        return pltpu.make_async_copy(stage.at[rows], out_ref.at[piece_rows(i, place * HALF)], keep_sem.at[lax.div(place, 2), i])

    def give_copy(j, i):
        return remote(stage.at[piece_rows(i, j * HALF)], out_ref.at[piece_rows(i, HALF)], out_ss.at[i], out_rs.at[i], mate)

    for order in range(3):
        j = jnp.where(chip == 0, (order + 2) % 3, order)
        place = 2 * (j - core)
        give = (place < 0) | (place > 2)

        def step(i, c):
            zx_copy(j, i).wait_recv()
            rows = sub_rows((3 * chip + j) * HALF, i)
            proj = (own[rows, :].astype(F32) + z_in[sub_rows(j * HALF, i), :].astype(F32)).astype(BF16).astype(F32)
            final = res[rows, :].astype(F32) + rms(proj, gain4).astype(BF16).astype(F32)
            stage[sub_rows(j * HALF, i), :] = final.astype(BF16)

            @pl.when(give)
            def _():
                give_copy(j, i).start()

            @pl.when(jnp.logical_not(give))
            def _():
                keep_copy(j, place, i).start()
            return c
        lax.fori_loop(0, PIECES, step, 0)

    for i in range(PIECES):
        give_copy(0, i).wait()
        keep_copy(0, 0, i).wait()
        keep_copy(0, 2, i).wait()
    zp_copy(N_CHUNK - 1).wait_send()
    for t in range(N_CHUNK):
        yx_copy(t).wait_send()
    for j in range(3):
        for i in range(PIECES):
            zx_copy(3 * (1 - chip) + j, i).wait_send()


def run_layer(block_rows, looked, tokens, k_pos, inv_freq, w_query, w_key, w_value, w_out, w_gate, w_up, w_down, g1, g2, g3, g4):
    seq, dim = looked.shape
    scale = float(np.sqrt(np.float32(dim)).astype(jnp.bfloat16))
    hbm = pl.BlockSpec(memory_space=pl.ANY)
    half_all = pltpu.VMEM((seq // 2, dim), BF16)
    dma = pltpu.SemaphoreType.DMA
    return pl.pallas_call(
        functools.partial(layer_kernel, block_rows, scale),
        name="layer",
        out_shape=jax.ShapeDtypeStruct((seq // 4, dim), BF16),
        in_specs=[hbm] * 15,
        out_specs=hbm,
        scratch_shapes=[
            pltpu.VMEM(tokens.shape, jnp.int32), pltpu.VMEM(k_pos.shape, jnp.int32), pltpu.VMEM(inv_freq.shape, F32),
            pltpu.VMEM((dim,), F32), pltpu.VMEM((dim,), F32), pltpu.VMEM((dim,), F32), pltpu.VMEM((dim,), F32),
            pltpu.VMEM((dim, 1024), BF16),
            pltpu.VMEM(w_out.shape, BF16), pltpu.VMEM(w_gate.shape, BF16), pltpu.VMEM(w_up.shape, BF16),
            pltpu.VMEM(w_down.shape, BF16),
            pltpu.VMEM((2, WQ_ROWS, 2, 256), BF16),
            half_all, half_all, half_all, half_all,
            pltpu.VMEM((4, ROWS, dim), BF16),
            pltpu.VMEM((seq, 256), BF16), pltpu.VMEM((seq, 256), BF16),
            pltpu.VMEM((ROWS, 512), BF16), pltpu.VMEM((ROWS, dim), BF16),
            pltpu.VMEM((HALF, dim), BF16), pltpu.VMEM((HALF, dim), BF16),
            pltpu.VMEM((HALF, dim), BF16), pltpu.VMEM((2, HALF, dim), BF16),
            pltpu.VMEM((3 * HALF, dim), BF16), pltpu.VMEM((3 * HALF, dim), BF16),
            dma((2,)), dma((6,)), dma((N_CHUNK,)), dma((N_CHUNK,)), dma((N_CHUNK,)), dma((N_CHUNK,)), dma((N_CHUNK,)),
            dma((2,)), dma((2,)), dma, dma,
            dma((N_CHUNK,)), dma((N_CHUNK,)), dma((2,)), dma((2,)), dma, dma((2,)),
            dma((3, PIECES)), dma((3, PIECES)), dma((PIECES,)), dma((PIECES,)), dma((2, PIECES)),
            dma((7,)), dma((PIECES,)), dma((PIECES,)), dma((PIECES,)), dma((PIECES,)), dma((PIECES,)),
        ],
        compiler_params=pltpu.CompilerParams(
            collective_id=0, has_side_effects=True, vmem_limit_bytes=67043328),
    )(looked, tokens, k_pos, inv_freq, w_query, w_key, w_value, w_out, w_gate, w_up, w_down, g1, g2, g3, g4)


def solution(mesh):
    in_specs = (P("dp", None), P("dp", None), P("tp", None), P(None, "tp", None), P(None, "tp", None), P(None, "tp", None), P("tp", None, None), P(None, "tp"), P(None, "tp"), P("tp", None), P(None), P(None), P(None), P(None))

    def device_step(tokens, positions, embed_block, w_query, w_key, w_value, w_out, w_gate, w_up, w_down, g1, g2, g3, g4):
        model_dim = embed_block.shape[1]
        block_rows = embed_block.shape[0]
        looked = embed_block.at[lax.rem(tokens[0], block_rows)].get(mode='promise_in_bounds')
        inv_freq = (ROPE_BASE ** (-2.0 * np.arange(128) / 256)).astype(np.float32).reshape(1, 128)
        out = run_layer(
            block_rows, looked, tokens, positions, jnp.asarray(inv_freq),
            w_query, w_key.reshape(model_dim, 256), w_value.reshape(model_dim, 256),
            w_out.reshape(512, model_dim), w_gate, w_up, w_down, g1, g2, g3, g4)
        return out[None]

    return jax.shard_map(device_step, mesh=mesh, in_specs=in_specs, out_specs=P("dp", "tp", None), check_vma=False)
```

```python
import functools

import jax
import jax.numpy as jnp
import numpy as np
from jax import lax
from jax.experimental import pallas as pl
from jax.experimental.pallas import tpu as pltpu
from jax.sharding import PartitionSpec as P

WINDOW = 4096
QUERY_SCALE = 256.0 ** -0.5
SOFT_CAP = 50.0
NORM_EPS = 1e-6
ROPE_BASE = 10000.0

N_CHUNK = 6
ROWS = 128
HALF = 64
SUB = 16
PIECES = 4
N_TILE = 512
WQ_ROWS = 256
EARLY = 2
LEAD = 3
LAG = 2
LATE = 4
MESH = pl.DeviceIdType.MESH
F32 = jnp.float32
BF16 = jnp.bfloat16


def rms(block, gain):
    mean_sq = jnp.mean(block * block, axis=-1, keepdims=True)
    return block * lax.rsqrt(mean_sq + NORM_EPS) * gain


def layer_kernel(
    block_rows, scale,
    rows_ref, ids_hbm, kpos_hbm, freq_hbm,
    wq_hbm, wk_hbm, wv_hbm, wo_hbm, wg_hbm, wu_hbm, wd_hbm,
    g1_hbm, g2_hbm, g3_hbm, g4_hbm,
    out_ref,
    ids_ref, kpos_ref, freq_ref, g1_ref, g2_ref, g3_ref, g4_ref,
    wqkv, wo, wg, wu, wd,
    wq_in, own, sib, res, y_in, norm, k_all, v_all, o_buf, h_buf, y_out, y_pair, pair_out, pair_in, z_in, stage,
    wq_sem, w_sem, own_sem, sib_ss, sib_rs, ex_ss, ex_rs, a_ss, a_rs, yp_ss, yp_rs,
    yx_ss, yx_rs, m_ss, m_rs, zp_ss, zp_rs, zx_ss, zx_rs, out_ss, out_rs, keep_sem,
    small_sem, stage_sem, first_ss, first_rs, ex0_ss, ex0_rs,
):
    dp = lax.axis_index("dp")
    tp = lax.axis_index("tp")
    chip = lax.div(tp, 2)
    core = lax.rem(tp, 2)
    mate = 2 * chip + 1 - core
    far = 2 * (1 - chip) + core

    def remote(src, dst, send_sem, recv_sem, target):
        return pltpu.make_async_remote_copy(
            src_ref=src, dst_ref=dst, send_sem=send_sem, recv_sem=recv_sem,
            device_id=(dp, target), device_id_type=MESH)

    def half_rows(t):
        return pl.ds(pl.multiple_of(t * HALF, HALF), HALF)

    mine = pl.ds(pl.multiple_of(core * HALF, HALF), HALF)

    def own_copy(t):
        rows = pl.ds(pl.multiple_of(t * ROWS + core * HALF, HALF), HALF)
        return pltpu.make_async_copy(rows_ref.at[rows], own.at[half_rows(t)], own_sem.at[t])

    def sib_copy(t):
        rows = pl.ds(pl.multiple_of(t * ROWS + (1 - core) * HALF, HALF), HALF)
        return remote(rows_ref.at[rows], sib.at[half_rows(t)], sib_ss.at[t], sib_rs.at[t], mate)

    def piece_rows(i, base=0):
        return pl.ds(pl.multiple_of(base + i * SUB, SUB), SUB)

    def stage_copy(i):
        rows = pl.ds(pl.multiple_of((1 - core) * HALF + i * SUB, SUB), SUB)
        return pltpu.make_async_copy(rows_ref.at[rows], y_out.at[piece_rows(i)], stage_sem.at[i])

    def sib_first(i):
        return remote(y_out.at[piece_rows(i)], sib.at[piece_rows(i)], first_ss.at[i], first_rs.at[i], mate)

    def ex_first(i):
        return remote(own.at[piece_rows(i)], res.at[piece_rows(i)], ex0_ss.at[i], ex0_rs.at[i], far)

    def ex_copy(t):
        return remote(own.at[half_rows(t)], res.at[half_rows(t)], ex_ss.at[t], ex_rs.at[t], far)

    def norm_copy(slot, send_sem, recv_sem):
        return remote(norm.at[slot, mine], norm.at[slot, mine], send_sem, recv_sem, mate)

    def yp_copy():
        return remote(y_out, y_pair, yp_ss, yp_rs, mate)

    def yx_copy(t):
        return remote(sib.at[half_rows(t)], y_in.at[half_rows(t)], yx_ss.at[t], yx_rs.at[t], far)

    def m_copy(t):
        slot = lax.rem(t, 2)
        return norm_copy(slot, m_ss.at[slot], m_rs.at[slot])

    def zp_copy(t):
        slot = lax.rem(t, 2)
        return remote(pair_out, pair_in.at[slot], zp_ss, zp_rs.at[slot], mate)

    def zx_copy(t, i):
        j = lax.rem(t, 3)
        return remote(own.at[piece_rows(i, t * HALF)], z_in.at[piece_rows(i, j * HALF)], zx_ss.at[j, i], zx_rs.at[j, i], far)

    weights = [
        pltpu.make_async_copy(src, dst, w_sem.at[i])
        for i, (src, dst) in enumerate(
            [(wk_hbm, wqkv.at[:, pl.ds(512, 256)]), (wv_hbm, wqkv.at[:, pl.ds(768, 256)]), (wo_hbm, wo), (wg_hbm, wg), (wu_hbm, wu), (wd_hbm, wd)])
    ]

    barrier = pltpu.get_barrier_semaphore()
    for peer in (far, mate):
        pl.semaphore_signal(barrier, inc=1, device_id=(dp, peer), device_id_type=MESH)
    for i in range(PIECES):
        stage_copy(i).start()
    own_copy(0).start()
    small = [
        pltpu.make_async_copy(src, dst, small_sem.at[i])
        for i, (src, dst) in enumerate([
            (ids_hbm, ids_ref), (kpos_hbm, kpos_ref), (freq_hbm, freq_ref),
            (g1_hbm, g1_ref), (g2_hbm, g2_ref), (g3_hbm, g3_ref), (g4_hbm, g4_ref)])
    ]
    for copy in small:
        copy.start()
    pl.semaphore_wait(barrier, 2)

    for i in range(PIECES):
        stage_copy(i).wait()
        sib_first(i).start()
    for t in range(1, N_CHUNK):
        sib_copy(t).start()
        own_copy(t).start()

    def wq_copy(i):
        slot = lax.rem(i, 2)
        rows = pl.ds(pl.multiple_of(i * WQ_ROWS, WQ_ROWS), WQ_ROWS)
        return pltpu.make_async_copy(wq_hbm.at[rows], wq_in.at[slot], wq_sem.at[slot])

    wq_copy(0).start()
    wq_copy(1).start()
    for copy in weights[:3]:
        copy.start()

    def sub_rows(base, i):
        return pl.ds(pl.multiple_of(base + i * SUB, SUB), SUB)

    def combine(dst, other, dst_base, other_base):
        def step(i, carry):
            rows = sub_rows(dst_base, i)
            total = dst[rows, :].astype(F32) + other[sub_rows(other_base, i), :].astype(F32)
            dst[rows, :] = total.astype(BF16)
            return carry
        lax.fori_loop(0, HALF // SUB, step, 0)

    def column(row_ref, t):
        rows = pl.ds(pl.multiple_of(t * ROWS, ROWS), ROWS)
        return jnp.broadcast_to(row_ref[:, rows], (8, ROWS)).T[:, :1]

    def owners(t):
        ids = column(ids_ref, t)
        ids = jnp.where(core == 0, ids[:HALF], ids[HALF:])
        local, local_mate = ids - tp * block_rows, ids - mate * block_rows
        held = (local >= 0) & (local < block_rows)
        held_mate = (local_mate >= 0) & (local_mate < block_rows)
        return held, held_mate

    def pick_rows(rows, held, held_mate):
        looked = jnp.where(held, own[rows, :].astype(F32), jnp.where(held_mate, sib[rows, :].astype(F32), 0.0))
        own[rows, :] = (looked * scale).astype(BF16)

    small[0].wait()
    held, held_mate = owners(0)
    own_copy(0).wait()
    for i in range(PIECES):
        part = slice(i * SUB, (i + 1) * SUB)
        sib_first(i).wait_recv()
        pick_rows(pl.ds(i * SUB, SUB), held[part], held_mate[part])
        ex_first(i).start()

    def send_embed(t, carry):
        held, held_mate = owners(t)
        own_copy(t).wait()
        sib_copy(t).wait_recv()
        for r in range(0, HALF, SUB):
            part = slice(r, r + SUB)
            pick_rows(pl.ds(pl.multiple_of(t * HALF + r, SUB), SUB), held[part], held_mate[part])

        @pl.when(t < LEAD)
        def _():
            ex_copy(t).start()
        return carry
    lax.fori_loop(1, N_CHUNK, send_embed, 0)

    for copy in small[1:]:
        copy.wait()
    k_all[...] = jnp.zeros_like(k_all)
    v_all[...] = jnp.zeros_like(v_all)
    gain1, gain2, gain3, gain4 = [(1.0 + g[...]).reshape(1, -1) for g in (g1_ref, g2_ref, g3_ref, g4_ref)]

    out_row = lax.broadcasted_iota(jnp.int32, (256, 256), 0)
    in_row = lax.broadcasted_iota(jnp.int32, (256, 256), 1)
    split_heads = jnp.where(in_row == jnp.where(out_row < 128, 2 * out_row, 2 * out_row - 255), 1.0, 0.0).astype(BF16)

    def spread_wq(i, carry):
        slot = lax.rem(i, 2)
        wq_copy(i).wait()
        for r in range(0, WQ_ROWS, 128):
            rows = pl.ds(pl.multiple_of(i * WQ_ROWS + r, 128), 128)
            both = wq_in[slot, r:r + 128].reshape(256, 256)
            both = jnp.dot(split_heads, both, preferred_element_type=F32).astype(BF16)
            wqkv[rows, :256] = both[:128]
            wqkv[rows, 256:512] = both[128:]

        @pl.when(i + 2 < 2560 // WQ_ROWS)
        def _():
            wq_copy(i + 2).start()
        return carry
    lax.fori_loop(0, 2560 // WQ_ROWS, spread_wq, 0)
    for copy in weights[3:]:
        copy.start()
    for i in range(PIECES):
        sib_first(i).wait_send()
    for t in range(1, N_CHUNK):
        sib_copy(t).wait_send()
    for copy in weights[:3]:
        copy.wait()

    def rope(states, cos_tab, sin_tab):
        lower, upper = states[:, :128], states[:, 128:]
        return lower * cos_tab - upper * sin_tab, upper * cos_tab + lower * sin_tab

    def split_halves(both):
        top, bottom = both[:HALF], both[HALF:]
        return jnp.where(core == 0, top, bottom), jnp.where(core == 0, bottom, top)

    def a_copy(t):
        slot = lax.rem(t, 2)
        return norm_copy(2 + slot, a_ss.at[slot], a_rs.at[slot])

    def embed_in(t):
        base = t * HALF
        slot = 2 + lax.rem(t, 2)

        @pl.when(t == 0)
        def _():
            for i in range(PIECES):
                ex_first(i).wait_recv()

        @pl.when(t > 0)
        def _():
            ex_copy(t).wait_recv()

        def embed_step(i, c):
            rows = sub_rows(base, i)
            embed = own[rows, :].astype(F32) + res[rows, :].astype(F32)
            res[rows, :] = embed.astype(BF16)
            norm[slot, sub_rows(core * HALF, i), :] = rms(embed, gain1).astype(BF16)
            return c
        lax.fori_loop(0, HALF // SUB, embed_step, 0)
        a_copy(t).start()

    def attention_chunk(t):
        slot = 2 + lax.rem(t, 2)
        rows = pl.ds(pl.multiple_of(t * ROWS, ROWS), ROWS)

        @pl.when(t <= LAG)
        def _():
            embed_in(t)
        q_pos = column(kpos_ref, t)
        angles = q_pos.astype(F32) * freq_ref[...]
        cos_tab, sin_tab = jnp.cos(angles), jnp.sin(angles)
        offset = q_pos - kpos_ref[...]
        keep = (offset >= 0) & (offset < WINDOW)
        a_copy(t).wait()
        proj = jnp.dot(norm[slot], wqkv[:, 512:], preferred_element_type=F32)
        lower, upper = rope(proj[:, :256], cos_tab, sin_tab)
        k_all[rows, :128] = lower.astype(BF16)
        k_all[rows, 128:] = upper.astype(BF16)
        v_all[rows, :] = proj[:, 256:].astype(BF16)
        proj = jnp.dot(norm[slot], wqkv[:, :512], preferred_element_type=F32)
        for head in range(2):
            lower, upper = rope(proj[:, head * 256:(head + 1) * 256], cos_tab, sin_tab)
            query = jnp.concatenate([(lower * QUERY_SCALE).astype(BF16), (upper * QUERY_SCALE).astype(BF16)], axis=-1)
            scores = lax.dot_general(query, k_all[...], (((1,), (1,)), ((), ())), preferred_element_type=F32)
            weight = jnp.where(keep, jnp.exp(SOFT_CAP * jnp.tanh(scores * (1.0 / SOFT_CAP))), 0.0)
            weight = weight * (1.0 / jnp.sum(weight, axis=-1, keepdims=True))
            mixed = jnp.dot(weight.astype(BF16), v_all[...], preferred_element_type=F32)
            o_buf[:, head * 256:(head + 1) * 256] = mixed.astype(BF16)

        def out_tile(n, c):
            cols = pl.ds(pl.multiple_of(n * N_TILE, N_TILE), N_TILE)
            both = jnp.dot(o_buf[...], wo[:, cols], preferred_element_type=F32).astype(BF16)
            sib[half_rows(t), cols], y_out[:, cols] = split_halves(both)
            return c
        lax.fori_loop(0, 2560 // N_TILE, out_tile, 0, unroll=True)
        yp_copy().start()

    def send_proj(t):
        yp_copy().wait()
        combine(sib, y_pair, t * HALF, 0)
        yx_copy(t).start()

        @pl.when(t + LEAD < N_CHUNK)
        def _():
            ex_copy(t + LEAD).start()

    def mlp_in(t):
        base = t * HALF
        slot = lax.rem(t, 2)
        yx_copy(t).wait_recv()

        def step(i, c):
            rows = sub_rows(base, i)
            proj = (sib[rows, :].astype(F32) + y_in[rows, :].astype(F32)).astype(BF16).astype(F32)
            resid = (res[rows, :].astype(F32) + rms(proj, gain2).astype(BF16).astype(F32)).astype(BF16)
            res[rows, :] = resid
            norm[slot, sub_rows(core * HALF, i), :] = rms(resid.astype(F32), gain3).astype(BF16)
            return c
        lax.fori_loop(0, HALF // SUB, step, 0)
        m_copy(t).start()

    def finish_pair(t):
        zp_copy(t).wait_recv()
        combine(own, pair_in.at[lax.rem(t, 2)], t * HALF, 0)

        @pl.when((lax.div(t, 3) != chip) & (t >= LAG))
        def _():
            for i in range(PIECES):
                zx_copy(t, i).start()

        @pl.when((t == LAG) & (chip != 0))
        def _():
            for early in range(LAG):
                for i in range(PIECES):
                    zx_copy(early, i).start()

    def mlp_chunk(t):
        slot = lax.rem(t, 2)

        @pl.when(t == 0)
        def _():
            for copy in weights[3:]:
                copy.wait()
            for i in range(PIECES):
                ex_first(i).wait_send()

        @pl.when(t > 0)
        def _():
            ex_copy(t).wait_send()
        m_copy(t).wait()

        def gate_tile(n, c):
            cols = pl.ds(pl.multiple_of(n * N_TILE, N_TILE), N_TILE)
            gate = jnp.dot(norm[slot], wg[:, cols], preferred_element_type=F32)
            up = jnp.dot(norm[slot], wu[:, cols], preferred_element_type=F32)
            h_buf[:, cols] = (jax.nn.gelu(gate, approximate=True) * up).astype(BF16)
            return c
        lax.fori_loop(0, EARLY, gate_tile, 0, unroll=True)

        @pl.when(t > 0)
        def _():
            finish_pair(t - 1)
        lax.fori_loop(EARLY, 2560 // N_TILE, gate_tile, 0, unroll=True)

        @pl.when(t + LAG + 1 < N_CHUNK)
        def _():
            embed_in(t + LAG + 1)

        @pl.when((t + 1 >= LATE) & (t < N_CHUNK - 1))
        def _():
            mlp_in(t + 1)

        @pl.when(t > 0)
        def _():
            zp_copy(t - 1).wait_send()

        def down_tile(n, c):
            cols = pl.ds(pl.multiple_of(n * N_TILE, N_TILE), N_TILE)
            both = jnp.dot(h_buf[...], wd[:, cols], preferred_element_type=F32).astype(BF16)
            own[half_rows(t), cols], pair_out[:, cols] = split_halves(both)
            return c
        lax.fori_loop(0, 2560 // N_TILE, down_tile, 0, unroll=True)
        zp_copy(t).start()

    def step(s, carry):
        @pl.when(s < N_CHUNK)
        def _():
            attention_chunk(s)

        @pl.when((s >= LAG) & (s < LATE + LAG))
        def _():
            mlp_in(s - LAG)

        @pl.when(s < N_CHUNK)
        def _():
            send_proj(s)

        @pl.when(s >= LAG)
        def _():
            mlp_chunk(s - LAG)
        return carry
    lax.fori_loop(0, N_CHUNK + LAG, step, 0)
    finish_pair(N_CHUNK - 1)

    def keep_copy(j, place, i):
        rows = piece_rows(i, j * HALF)
        return pltpu.make_async_copy(stage.at[rows], out_ref.at[piece_rows(i, place * HALF)], keep_sem.at[lax.div(place, 2), i])

    def give_copy(j, i):
        return remote(stage.at[piece_rows(i, j * HALF)], out_ref.at[piece_rows(i, HALF)], out_ss.at[i], out_rs.at[i], mate)

    for order in range(3):
        j = jnp.where(chip == 0, (order + 2) % 3, order)
        place = 2 * (j - core)
        give = (place < 0) | (place > 2)

        def step(i, c):
            zx_copy(j, i).wait_recv()
            rows = sub_rows((3 * chip + j) * HALF, i)
            proj = (own[rows, :].astype(F32) + z_in[sub_rows(j * HALF, i), :].astype(F32)).astype(BF16).astype(F32)
            final = res[rows, :].astype(F32) + rms(proj, gain4).astype(BF16).astype(F32)
            stage[sub_rows(j * HALF, i), :] = final.astype(BF16)

            @pl.when(give)
            def _():
                give_copy(j, i).start()

            @pl.when(jnp.logical_not(give))
            def _():
                keep_copy(j, place, i).start()
            return c
        lax.fori_loop(0, PIECES, step, 0)

    for i in range(PIECES):
        give_copy(0, i).wait()
        keep_copy(0, 0, i).wait()
        keep_copy(0, 2, i).wait()
    zp_copy(N_CHUNK - 1).wait_send()
    for t in range(N_CHUNK):
        yx_copy(t).wait_send()
    for j in range(3):
        for i in range(PIECES):
            zx_copy(3 * (1 - chip) + j, i).wait_send()


def run_layer(block_rows, looked, tokens, k_pos, inv_freq, w_query, w_key, w_value, w_out, w_gate, w_up, w_down, g1, g2, g3, g4):
    seq, dim = looked.shape
    scale = float(np.sqrt(np.float32(dim)).astype(jnp.bfloat16))
    hbm = pl.BlockSpec(memory_space=pl.ANY)
    half_all = pltpu.VMEM((seq // 2, dim), BF16)
    dma = pltpu.SemaphoreType.DMA
    return pl.pallas_call(
        functools.partial(layer_kernel, block_rows, scale),
        name="layer",
        out_shape=jax.ShapeDtypeStruct((seq // 4, dim), BF16),
        in_specs=[hbm] * 15,
        out_specs=hbm,
        scratch_shapes=[
            pltpu.VMEM(tokens.shape, jnp.int32), pltpu.VMEM(k_pos.shape, jnp.int32), pltpu.VMEM(inv_freq.shape, F32),
            pltpu.VMEM((dim,), F32), pltpu.VMEM((dim,), F32), pltpu.VMEM((dim,), F32), pltpu.VMEM((dim,), F32),
            pltpu.VMEM((dim, 1024), BF16),
            pltpu.VMEM(w_out.shape, BF16), pltpu.VMEM(w_gate.shape, BF16), pltpu.VMEM(w_up.shape, BF16),
            pltpu.VMEM(w_down.shape, BF16),
            pltpu.VMEM((2, WQ_ROWS, 2, 256), BF16),
            half_all, half_all, half_all, half_all,
            pltpu.VMEM((4, ROWS, dim), BF16),
            pltpu.VMEM((seq, 256), BF16), pltpu.VMEM((seq, 256), BF16),
            pltpu.VMEM((ROWS, 512), BF16), pltpu.VMEM((ROWS, dim), BF16),
            pltpu.VMEM((HALF, dim), BF16), pltpu.VMEM((HALF, dim), BF16),
            pltpu.VMEM((HALF, dim), BF16), pltpu.VMEM((2, HALF, dim), BF16),
            pltpu.VMEM((3 * HALF, dim), BF16), pltpu.VMEM((3 * HALF, dim), BF16),
            dma((2,)), dma((6,)), dma((N_CHUNK,)), dma((N_CHUNK,)), dma((N_CHUNK,)), dma((N_CHUNK,)), dma((N_CHUNK,)),
            dma((2,)), dma((2,)), dma, dma,
            dma((N_CHUNK,)), dma((N_CHUNK,)), dma((2,)), dma((2,)), dma, dma((2,)),
            dma((3, PIECES)), dma((3, PIECES)), dma((PIECES,)), dma((PIECES,)), dma((2, PIECES)),
            dma((7,)), dma((PIECES,)), dma((PIECES,)), dma((PIECES,)), dma((PIECES,)), dma((PIECES,)),
        ],
        compiler_params=pltpu.CompilerParams(
            collective_id=0, has_side_effects=True, vmem_limit_bytes=67043328),
    )(looked, tokens, k_pos, inv_freq, w_query, w_key, w_value, w_out, w_gate, w_up, w_down, g1, g2, g3, g4)


def solution(mesh):
    in_specs = (P("dp", None), P("dp", None), P("tp", None), P(None, "tp", None), P(None, "tp", None), P(None, "tp", None), P("tp", None, None), P(None, "tp"), P(None, "tp"), P("tp", None), P(None), P(None), P(None), P(None))

    def device_step(tokens, positions, embed_block, w_query, w_key, w_value, w_out, w_gate, w_up, w_down, g1, g2, g3, g4):
        model_dim = embed_block.shape[1]
        block_rows = embed_block.shape[0]
        looked = embed_block.at[lax.rem(tokens[0], block_rows)].get(mode='promise_in_bounds')
        inv_freq = (ROPE_BASE ** (-2.0 * np.arange(128) / 256)).astype(np.float32).reshape(1, 128)
        out = run_layer(
            block_rows, looked, tokens, positions, jnp.asarray(inv_freq),
            w_query, w_key.reshape(model_dim, 256), w_value.reshape(model_dim, 256),
            w_out.reshape(512, model_dim), w_gate, w_up, w_down, g1, g2, g3, g4)
        return out[None]

    return jax.shard_map(device_step, mesh=mesh, in_specs=in_specs, out_specs=P("dp", "tp", None), check_vma=False)
```
